32 devices in a mesh: tm: 4 (over y, core), space: 8 (over z, x).
Axes of the slice: x: 2, y: 2, z: 4, core: 2. Of those that a mesh axis runs over, the one named last changes fastest.
Arguments:
- perm_field: float32 [4, 32, 32, 256], P(None, 'space'), may hold values from 0.5 to 2
- step_multiplier: float32 [4, 32, 32, 256], P('tm', 'space'), may hold values from 0.5 to 2
- inflow: float32 [4, 32, 32, 256], P('tm', 'space'), may hold values from -3 to 3
- start_pressure: float32 [32, 32, 256], P('space'), may hold values from -6 to 6
- start_saturation: float32 [32, 32, 256], P('space'), may hold values from 0.1 to 0.9
- region_ids: int32 [32, 32, 256], P('space'), may hold values from 0 to 7
- region_table: float32 [3, 8], replicated, may hold values from 0.25 to 2
- well_cells: int32 [32], replicated, may hold values from 0 to 262143
- well_rates: float32 [4, 32], P('tm'), may hold values from -8 to 8
- observed: float32 [4, 4, 32], P(None, 'tm'), may hold values from -6 to 6
Outputs:
- misfit: float32 [4], replicated
- slab_pressure: float32 [4, 4, 32, 32, 256], P('tm', None, 'space')
- slab_saturation: float32 [4, 4, 32, 32, 256], P('tm', None, 'space')
The draws below stay inside these ranges and needn't reach their ends.
All inputs are finite; a program needn't handle non-finite values.
Results may differ from the reference program's by a relative error of at most 0.0003.
Values sent between devices are 32-bit elements; how exact they have to be, the bound alone decides.
A program may use at most 64 MiB of HBM per device.

```python
import math
import jax
import jax.numpy as jnp
from jax import lax

NZ = 32
NY = 256
REP_DEV = 1
ITERS = 3
WELLS = 32
REGIONS = 8
MEMBERS = 4
REPORTS = 4
NX = 32


def place_ends(entries, stream_key, low, largest):
    shape = entries.shape
    place = [jax.random.randint(jax.random.fold_in(stream_key, axis), (), 0, shape[axis]) for axis in range(len(shape))]
    entries = entries.at[tuple(place)].set(low)
    longest = shape.index(max(shape))
    place[longest] = (place[longest] + 1) % shape[longest]
    return entries.at[tuple(place)].set(largest)


def block_scale(key, extent, cuts, smallest, top_value):
    def one(dim, blocks):
        heights = jax.random.uniform(jax.random.fold_in(jax.random.fold_in(key, 6), dim), (blocks,), jnp.float32, smallest / len(cuts), top_value / len(cuts))
        return jnp.repeat(jnp.exp(heights), extent[dim] // blocks).reshape((-1,) + (1,) * (len(extent) - dim - 1))

    factor_of = one(*cuts[0])
    for cut in cuts[1:]:
        factor_of = factor_of * one(*cut)
    return factor_of


def bell_draw(rng, shape, scale, reach, shards=(), kind=jnp.bfloat16):
    values = scale * jax.random.normal(rng, shape, jnp.float32)
    if shards:
        values = values * block_scale(rng, shape, shards, -0.22, 0.18)
    return jnp.clip(values, -reach, reach).astype(kind)


def setup_inputs(seed: int = 0) -> dict:
    arg_keys = jax.random.split(jax.random.key(seed), 11)
    perm_field = jnp.clip(jnp.exp(math.log(2.0) - 1.3862944 * jax.random.uniform(arg_keys[0], (MEMBERS, NX, NZ, NY), jnp.float32) ** block_scale(arg_keys[0], (MEMBERS, NX, NZ, NY), ((1, 8),), -0.2, 0.2)), 0.5, 2.0)
    step_multiplier = jnp.clip(jnp.exp(math.log(2.0) - 1.3862944 * jax.random.uniform(arg_keys[1], (REPORTS, NX, NZ, NY), jnp.float32) ** block_scale(arg_keys[1], (REPORTS, NX, NZ, NY), ((0, 4), (1, 8)), -0.2, 0.2)), 0.5, 2.0)
    inflow = bell_draw(arg_keys[2], (REPORTS, NX, NZ, NY), 0.5, 3.0, ((0, 4), (1, 8)), jnp.float32)
    start_pressure = bell_draw(arg_keys[3], (NX, NZ, NY), 1.0, 6.0, ((0, 8),), jnp.float32)
    start_saturation = jnp.clip(0.1 + 0.79999997 * jax.random.uniform(arg_keys[4], (NX, NZ, NY), jnp.float32) ** block_scale(arg_keys[4], (NX, NZ, NY), ((0, 8),), -0.2, 0.2), 0.1, 0.9)
    region_ids = place_ends(jax.random.randint(arg_keys[5], (NX, NZ, NY), 0, REGIONS), jax.random.fold_in(arg_keys[5], 1), 0, REGIONS - 1).astype(jnp.int32)
    region_table = jnp.clip(jnp.exp(jax.random.uniform(arg_keys[6], (3, REGIONS), jnp.float32, math.log(0.25), math.log(2.0))), 0.25, 2.0)
    well_cells = place_ends(jax.random.randint(arg_keys[7], (WELLS,), 0, NX * NZ * NY), jax.random.fold_in(arg_keys[7], 1), 0, (NX * NZ * NY) - 1).astype(jnp.int32)
    well_rates = bell_draw(arg_keys[8], (REPORTS, WELLS), 2.0, 8.0, ((0, 4),), jnp.float32)
    observed = bell_draw(arg_keys[9], (MEMBERS, REPORTS, WELLS), 1.0, 6.0, ((1, 4),), jnp.float32)
    return {"perm_field": perm_field, "step_multiplier": step_multiplier, "inflow": inflow, "start_pressure": start_pressure, "start_saturation": start_saturation, "region_ids": region_ids, "region_table": region_table, "well_cells": well_cells, "well_rates": well_rates, "observed": observed}


def shifted(values, dimension, offset):
    margins = [(0, 0)] * values.ndim
    length = values.shape[dimension]
    if offset > 0:
        margins[dimension] = (1, 0)
        return lax.slice_in_dim(jnp.pad(values, margins), 0, length, axis=dimension)
    margins[dimension] = (0, 1)
    return lax.slice_in_dim(jnp.pad(values, margins), 1, length + 1, axis=dimension)

def neighbour_values(values_ext):
    middle = values_ext[:, 1:-1]
    return (values_ext[:, :-2], values_ext[:, 2:], shifted(middle, 2, 1), shifted(middle, 2, -1), shifted(middle, 3, 1), shifted(middle, 3, -1))

def coefficients(conduct_ext):
    middle = conduct_ext[:, 1:-1]
    others = neighbour_values(conduct_ext)
    links = [jnp.sqrt(middle * other_side) for other_side in others]
    link_total = links[0] + links[1] + links[2] + links[3] + links[4] + links[5]
    return tuple(links) + (link_total,)

def jacobi_sweep(pressure_ext, couplings, storage, right_side):
    beside = neighbour_values(pressure_ext)
    inflowing = couplings[0] * beside[0]
    for link_index in range(1, 6):
        inflowing = inflowing + couplings[link_index] * beside[link_index]
    divisor = jnp.where(storage > 0, storage + couplings[6], 1.0)
    return (right_side + inflowing) / divisor

def fraction(saturation, ratio):
    squared = saturation * saturation
    remain = (1.0 - saturation) * (1.0 - saturation)
    return squared / (squared + ratio * remain)

def transport(pressure_ext, flow_ext, couplings, saturation, gain, source):
    centre_p = pressure_ext[:, 1:-1]
    centre_f = flow_ext[:, 1:-1]
    other_p = neighbour_values(pressure_ext)
    other_f = neighbour_values(flow_ext)
    outflow = None
    for link_index in range(6):
        face_flux = couplings[link_index] * (centre_p - other_p[link_index])
        carried = face_flux * jnp.where(face_flux > 0, centre_f, other_f[link_index])
        outflow = carried if outflow is None else outflow + carried
    gained = jnp.maximum(source, 0.0) * (1.0 - saturation) - jnp.maximum(-source, 0.0) * centre_f - outflow
    return saturation + gain * gained

def region_fields(region_ids, region_table):
    fields = []
    for table_row in range(3):
        summed = jnp.zeros(region_ids.shape, jnp.float32)
        for region_index in range(region_table.shape[1]):
            summed = summed + jnp.where(region_ids == region_index, region_table[table_row, region_index], 0.0)
        fields.append(summed)
    return (fields[0], fields[1], 0.1 * fields[2])

def reference(perm_field, step_multiplier, inflow, start_pressure, start_saturation, region_ids, region_table, well_cells, well_rates, observed):
    storage, ratio, gain = region_fields(region_ids, region_table)
    pressure = jnp.broadcast_to(start_pressure, (MEMBERS,) + start_pressure.shape)
    saturation = jnp.broadcast_to(start_saturation, (MEMBERS,) + start_saturation.shape)
    misfit = jnp.zeros((MEMBERS,), jnp.float32)
    end_pressure = []
    end_saturation = []
    edges = ((0, 0), (1, 1), (0, 0), (0, 0))
    for report_index in range(REPORTS):
        source = jnp.zeros((NX * NZ * NY,), jnp.float32).at[well_cells].add(well_rates[report_index]).reshape(NX, NZ, NY)
        couplings = coefficients(jnp.pad(perm_field * step_multiplier[report_index], edges))
        right_side = storage * pressure + source + inflow[report_index]
        iterate = pressure
        for sweep_index in range(ITERS):
            iterate = jacobi_sweep(jnp.pad(iterate, edges), couplings, storage, right_side)
        flow_frac = fraction(saturation, ratio)
        saturation = transport(jnp.pad(iterate, edges), jnp.pad(flow_frac, edges), couplings, saturation, gain, source)
        pressure = iterate
        predicted = pressure.reshape(MEMBERS, -1)[:, well_cells]
        misfit = misfit + lax.optimization_barrier(jnp.sum((predicted - observed[:, report_index]) ** 2, axis=1))
        if (report_index + 1) % REP_DEV == 0:
            end_pressure.append(pressure)
            end_saturation.append(saturation)
    return (misfit / (REPORTS * WELLS), jnp.stack(end_pressure), jnp.stack(end_saturation))
```

```python
import functools

import jax
import jax.numpy as jnp
from jax import lax
from jax.experimental import pallas as pl
from jax.experimental.pallas import tpu as pltpu
from jax.sharding import PartitionSpec as P

ITERS = 3
H = ITERS + 1
MESH = pl.DeviceIdType.MESH
EXACT = lax.Precision.HIGHEST


def before(v, axis):
    return pltpu.roll(v, 1, axis)


def after(v, axis):
    return pltpu.roll(v, v.shape[axis] - 1, axis)


def kernel(
    T, N,
    perm, mult, infl, p0, s0, ids, table, small, rows_row,
    mis, outp, outs,
    PM, IDS, MS, IW, CW, SA, SO, PB, PX, SM, RC, SS, EE, QI, BB, DD, WW,
    IDW, SB, FE, HF, V, G, Q, ES, E0, E1, E2,
    lIN, sF, rF, sS, rS, sX, rX, sP, rP, sM, rM, sA, rA, sHF, rHF, sO, rO, lO, s1, r1, s2, r2,
):
    t = lax.axis_index("tm")
    i = lax.axis_index("space")
    X, Z, Y = IDS.shape
    R = T
    W = small.shape[0]
    U = N // 2
    XU = 2 * X
    WL = XU + 2 * H
    row = t // 2
    core = lax.rem(t, 2)
    u = i // 2
    h = lax.rem(i, 2)
    mate = t + 1 - 2 * core
    pair = i + 1 - 2 * h
    member = 2 * row + h
    own = H + h * X
    toward = 2 * h - 1
    side_here = (u > 0, u < U - 1)
    edge_there = jnp.logical_or(jnp.logical_and(h == 1, u < U - 1), jnp.logical_and(h == 0, u > 0))

    def load(n, src, dst):
        return pltpu.make_async_copy(src, dst, lIN.at[n])

    def rdma(src, dst, ss, rs, dev):
        return pltpu.make_async_remote_copy(
            src_ref=src, dst_ref=dst, send_sem=ss, recv_sem=rs, device_id=dev, device_id_type=MESH
        )

    mult_in = load(0, mult.at[0], MS.at[t])
    infl_in = load(1, infl.at[0], IW.at[t, pl.ds(own, X)])
    ids_in = load(2, ids, IDS)
    perm_in = load(3, perm.at[pl.ds(2 * row, 2)], PM)
    p0_in = load(4, p0, PB.at[0, pl.ds(own, X)])
    s0_in = load(3, s0, SB.at[0, pl.ds(h * X, X)])
    ids_win = load(4, ids, IDW.at[pl.ds(h * X, X)])
    mult_in.start()
    infl_in.start()

    @pl.when(core == 1)
    def _():
        perm_in.start()
        p0_in.start()
        ids_in.start()

    @pl.when(core == 0)
    def _():
        s0_in.start()
        ids_win.start()

    barrier = pltpu.get_barrier_semaphore()

    def greet(device):
        pl.semaphore_signal(barrier, inc=1, device_id=device, device_id_type=MESH)

    for d in range(1, T):
        peer = lax.rem(t + d, T)
        greet((peer, i))
        greet((peer, pair))
    for d in range(1, N):
        greet((t, lax.rem(i + d, N)))

    zi = lax.broadcasted_iota(jnp.int32, (Z, Y), 0)
    yi = lax.broadcasted_iota(jnp.int32, (Z, Y), 1)
    zero = jnp.zeros((Z, Y), jnp.float32)

    def neighbours(at, x):
        w = at(x)
        total = at(x - 1) + at(x + 1)
        total = total + (
            jnp.where(zi < Z - 1, after(w, 0), 0.0) + jnp.where(zi > 0, before(w, 0), 0.0)
        )
        return total + (
            jnp.where(yi < Y - 1, after(w, 1), 0.0) + jnp.where(yi > 0, before(w, 1), 0.0)
        )

    def looked_up(rock, which):
        v = zero
        for k in range(table.shape[1]):
            v = jnp.where(rock == k, table[which, k], v)
        return v

    lane = lax.broadcasted_iota(jnp.int32, (W, small.shape[1]), 1)

    def column(block, n):
        return jnp.sum(jnp.where(lane == n, block, 0.0), axis=1, keepdims=True)

    pick_cols = jnp.where(
        lax.broadcasted_iota(jnp.int32, (W, Y), 1).astype(jnp.float32) == column(small[...], T + 2),
        1.0, 0.0,
    )

    def put_rows(first, count):
        base = (first * Z).astype(jnp.float32)
        return jnp.where(
            lax.broadcasted_iota(jnp.int32, (count * Z, W), 0).astype(jnp.float32) == rows_row[...] - base,
            1.0, 0.0,
        )

    others_t = [(d, lax.rem(t + d, T)) for d in range(1, T)]

    def small_to(d, peer):
        return rdma(small, SM.at[t], sM.at[d], rM.at[t], (peer, i))

    def small_here(r):
        @pl.when(r != t)
        def _():
            rdma(SM.at[r], SM.at[r], sM.at[1], rM.at[r], (r, i)).wait_recv()

    def source(r, rows, count):
        rate = column(SM[r], 0)
        return jnp.dot(rows, pick_cols * rate, precision=EXACT).reshape(count, Z, Y)

    def field_to(rr):
        dev = (2 * rr + 1, i)
        return (
            rdma(MS.at[t], MS.at[t], sF.at[0, rr], rF.at[0, t], dev),
            rdma(
                IW.at[t, pl.ds(own, X)], IW.at[t, pl.ds(own, X)], sF.at[1, rr], rF.at[1, t], dev
            ),
        )

    def each_field(act):
        for rr in range(T // 2):
            @pl.when(t != 2 * rr + 1)
            def _():
                for copy in field_to(rr):
                    act(copy)

    def send_fields():
        each_field(lambda copy: copy.start())

    def put_out(r, half, src, which):
        dst = (outp, outs)[which].at[0, member]
        here = jnp.logical_and(r == t, half == h)

        @pl.when(jnp.logical_not(here))
        def _():
            rdma(src, dst, sO.at[r, half], rO.at[which, member], (r, 2 * u + half)).start()

        @pl.when(here)
        def _():
            pltpu.make_async_copy(src, dst, lO).start()

    def outs_sent(src, which):
        def sent(r, c):
            for half in (0, 1):
                dst = (outp, outs)[which].at[0, member]
                here = jnp.logical_and(r == t, half == h)

                @pl.when(jnp.logical_not(here))
                def _():
                    rdma(src, dst, sO.at[r, half], rO.at[which, member], (r, 2 * u + half)).wait_send()
            return c

        lax.fori_loop(0, R, sent, 0)
        pltpu.make_async_copy(src, (outp, outs)[which].at[0, member], lO).wait()

    def outs_here():
        for which in (0, 1):
            for m in range(T):
                mine = jnp.logical_and(core == 1 - which, m == member)

                @pl.when(jnp.logical_not(mine))
                def _():
                    dst = (outp, outs)[which].at[0, m]
                    rdma(dst, dst, sO.at[0, 0], rO.at[which, m], (t, pair)).wait_recv()

    def misfit_here(skip):
        for m in range(T):
            wait = rdma(E2.at[m], E2.at[m], s2.at[0], r2.at[m], (t, pair))
            if skip:
                @pl.when(m != member)
                def _():
                    wait.wait_recv()
            else:
                wait.wait_recv()
        lanes = lax.broadcasted_iota(jnp.int32, (8, 128), 1)
        result = jnp.zeros((8, 128), jnp.float32)
        for m in range(T):
            result = result + jnp.where(lanes == m, E2[m], 0.0)
        mis[...] = result * (1.0 / (R * W))

    def spread(n, window, depth, same, other):
        partner = rdma(
            other.at[pl.ds(0, X)], window.at[pl.ds(own, X)], sS.at[n, 0], rS.at[n, 0], (t, pair)
        )
        start = h * (X - depth)
        there = pl.ds((1 - h) * (H + XU) + h * (H - depth), depth)
        straight = rdma(
            same.at[pl.ds(start, depth)], window.at[there], sS.at[n, 1], rS.at[n, 2 - h],
            (t, i + 2 * toward),
        )
        aslant = rdma(
            other.at[pl.ds(start, depth)], window.at[there], sS.at[n, 2], rS.at[n, 2 - h],
            (t, i + toward),
        )
        return partner, straight, aslant

    def spread_start(*args):
        partner, straight, aslant = spread(*args)
        partner.start()

        @pl.when(edge_there)
        def _():
            straight.start()
            aslant.start()

    def spread_sent(*args):
        partner, straight, aslant = spread(*args)
        partner.wait_send()

        @pl.when(edge_there)
        def _():
            straight.wait_send()
            aslant.wait_send()

    def spread_here(n, window, depth):
        part = window.at[pl.ds(H + (1 - h) * X, X)]
        rdma(part, part, sS.at[n, 0], rS.at[n, 0], (t, pair)).wait_recv()
        for side in (0, 1):
            @pl.when(side_here[side])
            def _():
                part = window.at[pl.ds(H + XU if side else H - depth, depth)]
                rdma(part, part, sS.at[n, 1], rS.at[n, 1 + side], (t, pair)).wait_recv()

    def own_of(window):
        return window.at[pl.ds(own, X)]

    def conduct_args(r):
        return r, SA.at[r], H, own_of(SA.at[r]), SO.at[r]

    def inflow_args(r):
        mine = own_of(IW.at[r])
        return R + r, IW.at[r], H - 1, mine, mine

    def pressure_args():
        mine = own_of(PB.at[0])
        return 2 * R, PB.at[0], H, mine, mine

    def storage_args():
        mine = own_of(CW)
        return 2 * R + 1, CW, H - 1, mine, mine

    def distribute(r):
        @pl.when(r != t)
        def _():
            rdma(MS.at[r], MS.at[r], sF.at[0, 0], rF.at[0, r], (r, i)).wait_recv()

        for x in range(X):
            SO[r, x] = jnp.sqrt(PM[1 - h, x] * MS[r, x])
            SA[r, own + x] = jnp.sqrt(PM[h, x] * MS[r, x])
        spread_start(*conduct_args(r))

        @pl.when(r != t)
        def _():
            mine = own_of(IW.at[r])
            rdma(mine, mine, sF.at[1, 0], rF.at[1, r], (r, i)).wait_recv()
        spread_start(*inflow_args(r))

    def round_of(k, side):
        if side == 0:
            src, dst, dev = pl.ds(H, H), pl.ds(H + XU, H), (t, i - 2)
        else:
            src, dst, dev = pl.ds(XU, H), pl.ds(0, H), (t, i + 2)
        return rdma(PB.at[k, src], PB.at[k, dst], sP.at[k, side], rP.at[k, 1 - side], dev)

    def handed(r):
        mid = pl.ds(H, XU)
        wide = pl.ds(H - 1, XU + 2)
        dev = (mate, i)
        return (
            rdma(SA.at[r, wide], SA.at[r, wide], sX.at[r, 0], rX.at[r, 0], dev),
            rdma(PB.at[r + 1, mid], PB.at[r + 1, mid], sX.at[r, 1], rX.at[r, 1], dev),
            rdma(PX.at[r], PX.at[r], sX.at[r, 2], rX.at[r, 2], dev),
        )

    def meet():
        pl.semaphore_wait(barrier, (N - 1) + 2 * (T - 1))

    @pl.when(core == 1)
    def _():
        ids_in.wait()
        for x in range(X):
            CW[own + x] = looked_up(IDS[x], 0)
        for side in (0, 1):
            @pl.when(jnp.logical_not(side_here[side]))
            def _():
                first = H + XU if side else 0
                for x in range(first, first + H):
                    CW[x] = zero + 1.0

                def clear(r, c):
                    for x in range(first, first + H):
                        SA[r, x] = zero
                        IW[r, x] = zero
                        PB[r, x] = zero
                    return c

                lax.fori_loop(0, R, clear, 0)
        p0_in.wait()
        mult_in.wait()
        infl_in.wait()
        perm_in.wait()
        meet()
        spread_start(*pressure_args())
        spread_start(*storage_args())
        for d, peer in others_t:
            small_to(d, peer).start()
        SM[t] = small[...]
        distribute(0)
        send_fields()
        rows = put_rows(u * XU - H, WL)

        def coefficients(r):
            slot = lax.rem(r, 2)
            spread_here(r, SA.at[r], H)
            handed(r)[0].start()
            for x in range(1, WL - 1):
                a = SA[r, x]
                rc = 1.0 / (CW[x] + a * neighbours(lambda y: SA[r, y], x))
                RC[slot, x] = rc
                ss = a * rc
                SS[slot, x] = ss
                EE[slot, x] = a * ss
            small_here(r)
            q = source(r, rows, WL)
            spread_here(R + r, IW.at[r], H - 1)
            for x in range(1, WL - 1):
                QI[slot, x] = q[x] + IW[r, x]

        spread_here(2 * R, PB.at[0], H)
        spread_here(2 * R + 1, CW, H - 1)
        coefficients(0)
        distribute(1)

        def step(r, carry):
            slot = lax.rem(r, 2)

            def first(layers):
                for x in layers:
                    WW[0, x] = SA[r, x] * PB[r, x]

            def sweep_one(layers):
                for x in layers:
                    b = CW[x] * PB[r, x] + QI[slot, x]
                    d = SS[slot, x] * b
                    BB[x] = b
                    DD[x] = d
                    WW[1, x] = d + EE[slot, x] * neighbours(lambda y: WW[0, y], x)

            first(range(H, H + XU))
            sweep_one(range(H + 1, H + XU - 1))

            @pl.when(r > 0)
            def _():
                for side in (0, 1):
                    @pl.when(side_here[side])
                    def _():
                        part = PB.at[r, pl.ds(H + XU if side else 0, H)]
                        rdma(part, part, sP.at[r, side], rP.at[r, side], (t, pair)).wait_recv()

            first(range(0, H))
            sweep_one(range(1, H + 1))
            first(range(H + XU, WL))
            sweep_one(range(H + XU - 1, WL - 1))
            for j in range(1, ITERS - 1):
                for x in range(j + 1, WL - j - 1):
                    WW[j + 1, x] = DD[x] + EE[slot, x] * neighbours(lambda y: WW[j, y], x)

            def last(x):
                return RC[slot, x] * (
                    BB[x] + SA[r, x] * neighbours(lambda y: WW[ITERS - 1, y], x)
                )

            def send(side):
                @pl.when(jnp.logical_and(r < R - 1, side_here[side]))
                def _():
                    round_of(r + 1, side).start()

            for x in range(H, H + X):
                PB[r + 1, x] = last(x)
            send(0)
            for x in range(H + X, H + XU):
                PB[r + 1, x] = last(x)
            send(1)
            handed(r)[1].start()
            for half in (0, 1):
                put_out(r, half, PB.at[r + 1, pl.ds(H + half * X, X)], 0)
            PX[r, 0] = last(H - 1)
            PX[r, 1] = last(H + XU)
            handed(r)[2].start()

            @pl.when(r < R - 1)
            def _():
                coefficients(r + 1)

            @pl.when(r < R - 2)
            def _():
                distribute(r + 2)
            return carry

        lax.fori_loop(0, R, step, 0)
        misfit_here(False)
        outs_here()
        outs_sent(PB.at[0, pl.ds(0, X)], 0)

        def done(r, c):
            spread_sent(*conduct_args(r))
            spread_sent(*inflow_args(r))
            for copy in handed(r):
                copy.wait_send()

            @pl.when(r > 0)
            def _():
                for side in (0, 1):
                    @pl.when(side_here[side])
                    def _():
                        round_of(r, side).wait_send()
            return c

        lax.fori_loop(0, R, done, 0)
        spread_sent(*pressure_args())
        spread_sent(*storage_args())

    @pl.when(core == 0)
    def _():
        def fraction(s, v):
            sq = s * s
            rest = (1.0 - s) * (1.0 - s)
            return sq / (sq + v * rest)

        def edge_flow(r, side):
            src = FE.at[r, XU - 1 if side else 0]
            return rdma(
                src, HF.at[r, 1 - side], sHF.at[r, side], rHF.at[r, 1 - side], (t, i + 4 * side - 2)
            )

        def send_flow(r):
            for side in (0, 1):
                @pl.when(side_here[side])
                def _():
                    edge_flow(r, side).start()

        def pair_copies():
            part = pl.ds(h * X, X)
            return (
                rdma(SB.at[0, part], SB.at[0, part], sA.at[0], rA.at[0], (t, pair)),
                rdma(IDW.at[part], IDW.at[part], sA.at[1], rA.at[1], (t, pair)),
            )

        for side in (0, 1):
            @pl.when(jnp.logical_not(side_here[side]))
            def _():
                def clear(r, c):
                    HF[r, side] = zero
                    return c

                lax.fori_loop(0, R, clear, 0)

        mult_in.wait()
        infl_in.wait()
        s0_in.wait()
        ids_win.wait()
        meet()
        send_fields()
        for d, peer in others_t:
            small_to(d, peer).start()
        SM[t] = small[...]
        for copy in pair_copies():
            copy.start()
        rows = put_rows(u * XU, XU)
        local = column(small[...], T + 1) - (u * (XU * Z)).astype(jnp.float32)
        pick_rows = jnp.where(
            lax.broadcasted_iota(jnp.int32, (W, XU * Z), 1).astype(jnp.float32) == local, 1.0, 0.0
        )
        owned = jnp.sum(pick_rows, axis=1, keepdims=True)
        there = pl.ds((1 - h) * X, X)
        rdma(SB.at[0, there], SB.at[0, there], sA.at[0], rA.at[0], (t, pair)).wait_recv()
        rdma(IDW.at[there], IDW.at[there], sA.at[1], rA.at[1], (t, pair)).wait_recv()
        for x in range(XU):
            rock = IDW[x]
            V[x] = looked_up(rock, 1)
            G[x] = 0.1 * looked_up(rock, 2)
            FE[0, x] = fraction(SB[0, x], V[x])
        send_flow(0)
        ES[...] = jnp.zeros(ES.shape, jnp.float32)

        def step(r, carry):
            small_here(r)
            q_all = source(r, rows, XU)
            for x in range(XU):
                Q[x] = q_all[x]
            for copy in handed(r):
                copy.wait_recv()
            seen = jnp.dot(pick_rows, PB[r + 1, H:H + XU].reshape(XU * Z, Y), precision=EXACT)
            predicted = jnp.sum(seen * pick_cols, axis=1, keepdims=True)
            gap = predicted - column(SM[r], 1 + member)
            ES[...] = ES[...] + owned * gap * gap

            @pl.when(r == R - 1)
            def _():
                E0[...] = jnp.broadcast_to(jnp.sum(ES[...], axis=0, keepdims=True), E0.shape)
                for d in range(1, U):
                    peer = lax.rem(u + d, U)
                    rdma(E0, E1.at[u], s1.at[d], r1.at[u], (t, 2 * peer + h)).start()

            for side in (0, 1):
                @pl.when(side_here[side])
                def _():
                    part = HF.at[r, side]
                    rdma(part, part, sHF.at[r, side], rHF.at[r, side], (t, pair)).wait_recv()

            def p_of(x):
                return PX[r, 0] if x < 0 else (PX[r, 1] if x >= XU else PB[r + 1, H + x])

            def f_of(x):
                return HF[r, 0] if x < 0 else (HF[r, 1] if x >= XU else FE[r, x])

            def face(ai, aj, pi, pj, fi, fj):
                fall = pi - pj
                return ai * aj * fall * jnp.where(fall > 0, fi, fj)

            def across(x):
                return face(SA[r, H + x - 1], SA[r, H + x], p_of(x - 1), p_of(x), f_of(x - 1), f_of(x))

            low = across(0)
            for x in range(XU):
                high = across(x + 1)
                a = SA[r, H + x]
                p = p_of(x)
                f = f_of(x)
                s = SB[r, x]
                q = Q[x]
                cz = jnp.where(zi < Z - 1, face(a, after(a, 0), p, after(p, 0), f, after(f, 0)), 0.0)
                cy = jnp.where(yi < Y - 1, face(a, after(a, 1), p, after(p, 1), f, after(f, 1)), 0.0)
                out = (high - low) + (cz - before(cz, 0)) + (cy - before(cy, 1))
                low = high
                gained = jnp.maximum(q, 0.0) * (1.0 - s) - jnp.maximum(-q, 0.0) * f - out
                s = s + G[x] * gained
                SB[r + 1, x] = s
                FE[r + 1, x] = fraction(s, V[x])
                if x == X - 1:
                    put_out(r, 0, SB.at[r + 1, pl.ds(0, X)], 1)
            put_out(r, 1, SB.at[r + 1, pl.ds(X, X)], 1)

            @pl.when(r < R - 1)
            def _():
                send_flow(r + 1)
            return carry

        lax.fori_loop(0, R, step, 0)
        E1[u] = E0[...]
        for d in range(1, U):
            peer = lax.rem(u + d, U)
            rdma(E1.at[peer], E1.at[peer], s1.at[d], r1.at[peer], (t, pair)).wait_recv()
        whole = E1[0]
        for n in range(1, U):
            whole = whole + E1[n]
        E2[member] = whole

        def plane(act):
            n = 0
            for d in range(T):
                for half in (0, 1):
                    if d == 0 and half == 0:
                        continue
                    dev = (lax.rem(t + d, T), i if half == 0 else pair)
                    act(rdma(E2.at[member], E2.at[member], s2.at[n], r2.at[member], dev))
                    n += 1

        plane(lambda copy: copy.start())
        misfit_here(True)
        outs_here()
        outs_sent(SB.at[0, pl.ds(0, X)], 1)
        plane(lambda copy: copy.wait_send())
        for d in range(1, U):
            peer = lax.rem(u + d, U)
            rdma(E0, E1.at[u], s1.at[d], r1.at[u], (t, 2 * peer + h)).wait_send()
        for copy in pair_copies():
            copy.wait_send()

        def done(r, c):
            for side in (0, 1):
                @pl.when(side_here[side])
                def _():
                    edge_flow(r, side).wait_send()
            return c

        lax.fori_loop(0, R, done, 0)

    each_field(lambda copy: copy.wait_send())
    for d, peer in others_t:
        small_to(d, peer).wait_send()


def body(
    perm_field, step_multiplier, inflow, start_pressure, start_saturation,
    region_ids, region_table, well_cells, well_rates, observed,
):
    T = lax.axis_size("tm")
    N = lax.axis_size("space")
    X, Z, Y = start_pressure.shape
    W = well_cells.shape[0]
    members = perm_field.shape[0]
    assert members == T and T % 2 == 0 and N % 2 == 0 and X >= H and step_multiplier.shape[0] == 1
    well_row = (well_cells // Y).astype(jnp.float32)
    well_col = (well_cells % Y).astype(jnp.float32)
    small = jnp.concatenate(
        [well_rates, observed[:, 0, :], well_row[None], well_col[None]], axis=0
    ).T
    small = jnp.pad(small, ((0, 0), (0, 128 - small.shape[1])))
    R = T
    U = N // 2
    XU = 2 * X
    WL = XU + 2 * H
    f32 = jnp.float32
    cell = (Z, Y)
    block = (X, Z, Y)
    window = (WL, Z, Y)
    unit = (XU, Z, Y)

    def buf(*shape):
        return pltpu.VMEM(shape, f32)

    dma = pltpu.SemaphoreType.DMA
    vmem = pl.BlockSpec(memory_space=pltpu.VMEM)
    anyspace = pl.BlockSpec(memory_space=pl.ANY)
    out_shape = jax.ShapeDtypeStruct((1, members) + block, f32)
    mis, outp, outs = pl.pallas_call(
        functools.partial(kernel, T, N),
        out_shape=(jax.ShapeDtypeStruct((8, 128), f32), out_shape, out_shape),
        in_specs=[anyspace] * 6 + [pl.BlockSpec(memory_space=pltpu.SMEM)] + [vmem] * 2,
        out_specs=(vmem, anyspace, anyspace),
        scratch_shapes=[
            buf(2, *block), pltpu.VMEM(block, jnp.int32), buf(R, *block), buf(R, *window), buf(*window),
            buf(R, *window), buf(R, *block), buf(R + 1, *window), buf(R, 2, *cell), buf(T, W, 128),
            buf(2, *window), buf(2, *window), buf(2, *window), buf(2, *window), buf(*window),
            buf(*window), buf(ITERS, *window),
            pltpu.VMEM(unit, jnp.int32), buf(R + 1, *unit), buf(R + 1, *unit), buf(R, 2, *cell),
            buf(*unit), buf(*unit), buf(*unit), buf(W, 1), buf(8, 128), buf(U, 8, 128), buf(T, 8, 128),
            dma((5,)), dma((2, T // 2)), dma((2, T)), dma((2 * R + 2, 3)), dma((2 * R + 2, 3)),
            dma((R, 3)), dma((R, 3)), dma((R + 1, 2)), dma((R + 1, 2)), dma((T,)), dma((T,)),
            dma((2,)), dma((2,)), dma((R, 2)), dma((R, 2)),
            dma((R, 2)), dma((2, T)), dma(()), dma((max(U, 2),)), dma((U,)), dma((2 * T - 1,)), dma((T,)),
        ],
        compiler_params=pltpu.CompilerParams(
            has_side_effects=True, collective_id=0, vmem_limit_bytes=56 * 1024 * 1024
        ),
    )(
        perm_field, step_multiplier, inflow, start_pressure, start_saturation, region_ids,
        region_table, small, well_row[None],
    )
    return mis[0, :members], outp, outs


def solution(mesh):
    return jax.shard_map(
        body,
        mesh=mesh,
        in_specs=(
            P(None, "space", None, None),
            P("tm", "space", None, None),
            P("tm", "space", None, None),
            P("space", None, None),
            P("space", None, None),
            P("space", None, None),
            P(),
            P(),
            P("tm", None),
            P(None, "tm", None),
        ),
        out_specs=(P(), P("tm", None, "space", None, None), P("tm", None, "space", None, None)),
        check_vma=False,
    )
```

```python
import functools

import jax
import jax.numpy as jnp
from jax import lax
from jax.experimental import pallas as pl
from jax.experimental.pallas import tpu as pltpu
from jax.sharding import PartitionSpec as P

ITERS = 3
H = ITERS + 1
MESH = pl.DeviceIdType.MESH
EXACT = lax.Precision.HIGHEST


def before(v, axis):
    return pltpu.roll(v, 1, axis)


def after(v, axis):
    return pltpu.roll(v, v.shape[axis] - 1, axis)


def kernel(
    T, N,
    perm, mult, infl, p0, s0, ids, table, cells, rates, seen_in,
    mis, outp, outs,
    PM, IDS, MS, IW, CW, SA, SO, PB, PX, SM, RC, SS, EE, QI, BB, DD, WW,
    IDW, SB, FE, HF, V, G, Q, ES, E0, E1, E2,
    lIN, sF, rF, sS, rS, sX, rX, sP, rP, sM, rM, sA, rA, sHF, rHF, sO, rO, lO, s1, r1, s2, r2, go,
):
    t = lax.axis_index("tm")
    i = lax.axis_index("space")
    X, Z, Y = IDS.shape
    R = T
    W = cells.shape[1]
    U = N // 2
    XU = 2 * X
    WL = XU + 2 * H
    row = t // 2
    core = lax.rem(t, 2)
    u = i // 2
    h = lax.rem(i, 2)
    mate = t + 1 - 2 * core
    pair = i + 1 - 2 * h
    member = 2 * row + h
    own = H + h * X
    side_here = (u > 0, u < U - 1)

    def load(n, src, dst):
        return pltpu.make_async_copy(src, dst, lIN.at[n])

    def rdma(src, dst, ss, rs, dev):
        return pltpu.make_async_remote_copy(
            src_ref=src, dst_ref=dst, send_sem=ss, recv_sem=rs, device_id=dev, device_id_type=MESH
        )

    mult_in = load(0, mult.at[0], MS.at[t])
    infl_in = load(1, infl.at[0], IW.at[t, pl.ds(own, X)])
    ids_in = load(2, ids, IDS)
    perm_in = load(3, perm.at[pl.ds(2 * row, 2)], PM)
    p0_in = load(4, p0, PB.at[0, pl.ds(own, X)])
    s0_in = load(3, s0, SB.at[0, pl.ds(h * X, X)])
    ids_win = load(4, ids, IDW.at[pl.ds(h * X, X)])
    mult_in.start()
    infl_in.start()

    @pl.when(core == 1)
    def _():
        perm_in.start()
        p0_in.start()
        ids_in.start()

    @pl.when(core == 0)
    def _():
        s0_in.start()
        ids_win.start()

    barrier = pltpu.get_barrier_semaphore()

    def greet(device):
        pl.semaphore_signal(barrier, inc=1, device_id=device, device_id_type=MESH)

    for d in range(1, T):
        peer = lax.rem(t + d, T)
        greet((peer, i))
        greet((peer, pair))
    for d in range(1, N):
        greet((t, lax.rem(i + d, N)))

    zi = lax.broadcasted_iota(jnp.int32, (Z, Y), 0)
    yi = lax.broadcasted_iota(jnp.int32, (Z, Y), 1)
    zero = jnp.zeros((Z, Y), jnp.float32)

    def neighbours(at, x):
        w = at(x)
        total = at(x - 1) + at(x + 1)
        total = total + (
            jnp.where(zi < Z - 1, after(w, 0), 0.0) + jnp.where(zi > 0, before(w, 0), 0.0)
        )
        return total + (
            jnp.where(yi < Y - 1, after(w, 1), 0.0) + jnp.where(yi > 0, before(w, 1), 0.0)
        )

    def looked_up(rock, which):
        v = zero
        for k in range(table.shape[1]):
            v = jnp.where(rock == k, table[which, k], v)
        return v

    def upright(line):
        eye = lax.broadcasted_iota(jnp.int32, (W, W), 0) == lax.broadcasted_iota(jnp.int32, (W, W), 1)
        return jnp.sum(jnp.where(eye, line, 0.0), axis=1, keepdims=True)

    bits = Y.bit_length() - 1
    rows_row = jnp.right_shift(cells[...], bits).astype(jnp.float32)
    cols_row = jnp.bitwise_and(cells[...], Y - 1).astype(jnp.float32)
    pick_cols = jnp.where(
        lax.broadcasted_iota(jnp.int32, (W, Y), 1).astype(jnp.float32) == upright(cols_row), 1.0, 0.0
    )
    SM[t] = jnp.zeros(SM.shape[1:], jnp.float32)
    SM[t, 0:1, 0:W] = rates[...]
    SM[t, 1:1 + T, 0:W] = seen_in[...]

    def put_rows(first, count):
        base = (first * Z).astype(jnp.float32)
        return jnp.where(
            lax.broadcasted_iota(jnp.int32, (count * Z, W), 0).astype(jnp.float32) == rows_row - base,
            1.0, 0.0,
        )

    others_t = [(d, lax.rem(t + d, T)) for d in range(1, T)]

    def small_to(d, peer):
        return rdma(SM.at[t], SM.at[t], sM.at[d], rM.at[t], (peer, i))

    def small_here(r):
        @pl.when(r != t)
        def _():
            rdma(SM.at[r], SM.at[r], sM.at[1], rM.at[r], (r, i)).wait_recv()

    def source(r, rows, count):
        rate = upright(SM[r, 0:1, 0:W])
        return jnp.dot(rows, pick_cols * rate, precision=EXACT).reshape(count, Z, Y)

    def field_to(rr):
        dev = (2 * rr + 1, i)
        return (
            rdma(MS.at[t], MS.at[t], sF.at[0, rr], rF.at[0, t], dev),
            rdma(
                IW.at[t, pl.ds(own, X)], IW.at[t, pl.ds(own, X)], sF.at[1, rr], rF.at[1, t], dev
            ),
        )

    def each_field(act):
        for rr in range(T // 2):
            @pl.when(t != 2 * rr + 1)
            def _():
                for copy in field_to(rr):
                    act(copy)

    def send_fields():
        each_field(lambda copy: copy.start())

    def put_out(r, half, src, which):
        dst = (outp, outs)[which].at[0, member]
        here = jnp.logical_and(r == t, half == h)

        @pl.when(jnp.logical_not(here))
        def _():
            rdma(src, dst, sO.at[r, half], rO.at[which, member], (r, 2 * u + half)).start()

        @pl.when(here)
        def _():
            pltpu.make_async_copy(src, dst, lO).start()

    def outs_sent(src, which):
        def sent(r, c):
            for half in (0, 1):
                dst = (outp, outs)[which].at[0, member]
                here = jnp.logical_and(r == t, half == h)

                @pl.when(jnp.logical_not(here))
                def _():
                    rdma(src, dst, sO.at[r, half], rO.at[which, member], (r, 2 * u + half)).wait_send()
            return c

        lax.fori_loop(0, R, sent, 0)
        pltpu.make_async_copy(src, (outp, outs)[which].at[0, member], lO).wait()

    def outs_here():
        for which in (0, 1):
            for m in range(T):
                mine = jnp.logical_and(core == 1 - which, m == member)

                @pl.when(jnp.logical_not(mine))
                def _():
                    dst = (outp, outs)[which].at[0, m]
                    rdma(dst, dst, sO.at[0, 0], rO.at[which, m], (t, pair)).wait_recv()

    def misfit_here(skip):
        for m in range(T):
            wait = rdma(E2.at[m], E2.at[m], s2.at[0], r2.at[m], (t, pair))
            if skip:
                @pl.when(m != member)
                def _():
                    wait.wait_recv()
            else:
                wait.wait_recv()
        lanes = lax.broadcasted_iota(jnp.int32, (8, 128), 1)
        result = jnp.zeros((8, 128), jnp.float32)
        for m in range(T):
            result = result + jnp.where(lanes == m, E2[m], 0.0)
        mis[...] = result * (1.0 / (R * W))

    def edge_of(side, depth):
        src = pl.ds(H + XU - depth if side else H, depth)
        dst = pl.ds(H - depth if side else H + XU, depth)
        return src, dst

    def pooled(n, window, other):
        return rdma(
            other.at[pl.ds(0, X)], window.at[pl.ds(own, X)], sS.at[n, 0], rS.at[n, 0], (t, pair)
        )

    def halo(n, window, depth, side, relayed):
        src, dst = edge_of(side, depth)
        return rdma(
            window.at[src], window.at[dst], sS.at[n, 1 + relayed], rS.at[n, 2 - side],
            (t, i + 4 * side - 2),
        )

    def halos(n, window, depth, relayed, act):
        for side in (0, 1):
            @pl.when(jnp.logical_and(side_here[side], h == (1 - side if relayed else side)))
            def _():
                act(halo(n, window, depth, side, relayed))

    def pool(n, window, depth, other):
        pooled(n, window, other).start()
        halos(n, window, depth, 0, lambda copy: copy.start())

    def relay(n, window, depth, other):
        part = window.at[pl.ds(H + (1 - h) * X, X)]
        rdma(part, part, sS.at[n, 0], rS.at[n, 0], (t, pair)).wait_recv()
        halos(n, window, depth, 1, lambda copy: copy.start())

    def spread_here(n, window, depth, other):
        for side in (0, 1):
            @pl.when(side_here[side])
            def _():
                part = window.at[pl.ds(H + XU if side else H - depth, depth)]
                rdma(part, part, sS.at[n, 1], rS.at[n, 1 + side], (t, pair)).wait_recv()

    def spread_sent(n, window, depth, other):
        pooled(n, window, other).wait_send()
        for relayed in (0, 1):
            halos(n, window, depth, relayed, lambda copy: copy.wait_send())

    def own_of(window):
        return window.at[pl.ds(own, X)]

    def conduct_args(r):
        return r, SA.at[r], H, SO.at[r]

    def inflow_args(r):
        return R + r, IW.at[r], H - 1, own_of(IW.at[r])

    def pressure_args():
        return 2 * R, PB.at[0], H, own_of(PB.at[0])

    def storage_args():
        return 2 * R + 1, CW, H - 1, own_of(CW)

    def distribute(r):
        @pl.when(r != t)
        def _():
            rdma(MS.at[r], MS.at[r], sF.at[0, 0], rF.at[0, r], (r, i)).wait_recv()

        for x in range(X):
            SO[r, x] = jnp.sqrt(PM[1 - h, x] * MS[r, x])
            SA[r, own + x] = jnp.sqrt(PM[h, x] * MS[r, x])
        pool(*conduct_args(r))

        @pl.when(r != t)
        def _():
            mine = own_of(IW.at[r])
            rdma(mine, mine, sF.at[1, 0], rF.at[1, r], (r, i)).wait_recv()
        pool(*inflow_args(r))

    def round_of(k, side):
        if side == 0:
            src, dst, dev = pl.ds(H, H), pl.ds(H + XU, H), (t, i - 2)
        else:
            src, dst, dev = pl.ds(XU, H), pl.ds(0, H), (t, i + 2)
        return rdma(PB.at[k, src], PB.at[k, dst], sP.at[k, side], rP.at[k, 1 - side], dev)

    def handed(r):
        mid = pl.ds(H, XU)
        wide = pl.ds(H - 1, XU + 2)
        dev = (mate, i)
        return (
            rdma(SA.at[r, wide], SA.at[r, wide], sX.at[r, 0], rX.at[r, 0], dev),
            rdma(PB.at[r + 1, mid], PB.at[r + 1, mid], sX.at[r, 1], rX.at[r, 1], dev),
            rdma(PX.at[r], PX.at[r], sX.at[r, 2], rX.at[r, 2], dev),
        )

    def meet():
        pl.semaphore_wait(barrier, (N - 1) + 2 * (T - 1))

    @pl.when(core == 1)
    def _():
        ids_in.wait()
        for x in range(X):
            CW[own + x] = looked_up(IDS[x], 0)
        for side in (0, 1):
            @pl.when(jnp.logical_not(side_here[side]))
            def _():
                first = H + XU if side else 0
                for x in range(first, first + H):
                    CW[x] = zero + 1.0

                def clear(r, c):
                    for x in range(first, first + H):
                        SA[r, x] = zero
                        IW[r, x] = zero
                        PB[r, x] = zero
                    return c

                lax.fori_loop(0, R, clear, 0)
        p0_in.wait()
        mult_in.wait()
        infl_in.wait()
        perm_in.wait()
        meet()
        pool(*pressure_args())
        pool(*storage_args())
        for d, peer in others_t:
            small_to(d, peer).start()
        distribute(0)
        pl.semaphore_signal(go, inc=1, device_id=(mate, i), device_id_type=MESH)
        send_fields()
        rows = put_rows(u * XU - H, WL)
        local = upright(rows_row) - (u * (XU * Z)).astype(jnp.float32)
        pick_rows = jnp.where(
            lax.broadcasted_iota(jnp.int32, (W, XU * Z), 1).astype(jnp.float32) == local, 1.0, 0.0
        )
        owned = jnp.sum(pick_rows, axis=1, keepdims=True)
        ES[...] = jnp.zeros(ES.shape, jnp.float32)

        def coefficients(r):
            slot = lax.rem(r, 2)
            spread_here(*conduct_args(r))
            handed(r)[0].start()
            for x in range(1, WL - 1):
                a = SA[r, x]
                rc = 1.0 / (CW[x] + a * neighbours(lambda y: SA[r, y], x))
                RC[slot, x] = rc
                ss = a * rc
                SS[slot, x] = ss
                EE[slot, x] = a * ss
            small_here(r)
            q = source(r, rows, WL)
            spread_here(*inflow_args(r))
            for x in range(1, WL - 1):
                QI[slot, x] = q[x] + IW[r, x]

        def relay_fields(r):
            relay(*conduct_args(r))
            relay(*inflow_args(r))

        relay(*pressure_args())
        relay(*storage_args())
        relay_fields(0)
        distribute(1)
        spread_here(*pressure_args())
        spread_here(*storage_args())
        coefficients(0)
        relay_fields(1)
        if R > 2:
            distribute(2)

        def step(r, carry):
            slot = lax.rem(r, 2)

            def first(layers):
                for x in layers:
                    WW[0, x] = SA[r, x] * PB[r, x]

            def sweep_one(layers):
                for x in layers:
                    b = CW[x] * PB[r, x] + QI[slot, x]
                    d = SS[slot, x] * b
                    BB[x] = b
                    DD[x] = d
                    WW[1, x] = d + EE[slot, x] * neighbours(lambda y: WW[0, y], x)

            first(range(H, H + XU))
            sweep_one(range(H + 1, H + XU - 1))

            @pl.when(r > 0)
            def _():
                for side in (0, 1):
                    @pl.when(side_here[side])
                    def _():
                        part = PB.at[r, pl.ds(H + XU if side else 0, H)]
                        rdma(part, part, sP.at[r, side], rP.at[r, side], (t, pair)).wait_recv()

            first(range(0, H))
            sweep_one(range(1, H + 1))
            first(range(H + XU, WL))
            sweep_one(range(H + XU - 1, WL - 1))
            for j in range(1, ITERS - 1):
                for x in range(j + 1, WL - j - 1):
                    WW[j + 1, x] = DD[x] + EE[slot, x] * neighbours(lambda y: WW[j, y], x)

            def last(x):
                return RC[slot, x] * (
                    BB[x] + SA[r, x] * neighbours(lambda y: WW[ITERS - 1, y], x)
                )

            def send(side):
                @pl.when(jnp.logical_and(r < R - 1, side_here[side]))
                def _():
                    round_of(r + 1, side).start()

            for x in range(H, H + X):
                PB[r + 1, x] = last(x)
            send(0)
            for x in range(H + X, H + XU):
                PB[r + 1, x] = last(x)
            send(1)
            handed(r)[1].start()
            for half in (0, 1):
                put_out(r, half, PB.at[r + 1, pl.ds(H + half * X, X)], 0)
            PX[r, 0] = last(H - 1)
            PX[r, 1] = last(H + XU)
            handed(r)[2].start()
            seen = jnp.dot(pick_rows, PB[r + 1, H:H + XU].reshape(XU * Z, Y), precision=EXACT)
            predicted = jnp.sum(seen * pick_cols, axis=1, keepdims=True)
            lines = lax.broadcasted_iota(jnp.int32, SM.shape[1:], 0)
            seen_row = jnp.sum(jnp.where(lines == 1 + member, SM[r], 0.0), axis=0, keepdims=True)
            gap = predicted - upright(seen_row[:, :W])
            ES[...] = ES[...] + owned * gap * gap

            @pl.when(r == R - 1)
            def _():
                E0[...] = jnp.broadcast_to(jnp.sum(ES[...], axis=0, keepdims=True), E0.shape)
                for d in range(1, U):
                    peer = lax.rem(u + d, U)
                    rdma(E0, E1.at[u], s1.at[d], r1.at[u], (t, 2 * peer + h)).start()

            @pl.when(r < R - 1)
            def _():
                coefficients(r + 1)

            @pl.when(r < R - 2)
            def _():
                relay_fields(r + 2)

            @pl.when(r < R - 3)
            def _():
                distribute(r + 3)
            return carry

        lax.fori_loop(0, R, step, 0)
        E1[u] = E0[...]
        for d in range(1, U):
            peer = lax.rem(u + d, U)
            rdma(E1.at[peer], E1.at[peer], s1.at[d], r1.at[peer], (t, pair)).wait_recv()
        whole = E1[0]
        for n in range(1, U):
            whole = whole + E1[n]
        E2[member] = whole

        def plane(act):
            n = 0
            for d in range(T):
                for half in (0, 1):
                    if d == 0 and half == 0:
                        continue
                    dev = (lax.rem(t + d, T), i if half == 0 else pair)
                    act(rdma(E2.at[member], E2.at[member], s2.at[n], r2.at[member], dev))
                    n += 1

        plane(lambda copy: copy.start())
        misfit_here(True)
        outs_here()
        outs_sent(PB.at[0, pl.ds(0, X)], 0)
        plane(lambda copy: copy.wait_send())
        for d in range(1, U):
            peer = lax.rem(u + d, U)
            rdma(E0, E1.at[u], s1.at[d], r1.at[u], (t, 2 * peer + h)).wait_send()

        def done(r, c):
            spread_sent(*conduct_args(r))
            spread_sent(*inflow_args(r))
            for copy in handed(r):
                copy.wait_send()

            @pl.when(r > 0)
            def _():
                for side in (0, 1):
                    @pl.when(side_here[side])
                    def _():
                        round_of(r, side).wait_send()
            return c

        lax.fori_loop(0, R, done, 0)
        spread_sent(*pressure_args())
        spread_sent(*storage_args())

    @pl.when(core == 0)
    def _():
        def fraction(s, v):
            sq = s * s
            rest = (1.0 - s) * (1.0 - s)
            return sq / (sq + v * rest)

        def edge_flow(r, side):
            src = FE.at[r, XU - 1 if side else 0]
            return rdma(
                src, HF.at[r, 1 - side], sHF.at[r, side], rHF.at[r, 1 - side], (t, i + 4 * side - 2)
            )

        def first_flow(act):
            for side in (0, 1):
                @pl.when(jnp.logical_and(side_here[side], h == side))
                def _():
                    src = FE.at[0, XU - 1 if side else 0]
                    for n, hop in ((0, 2), (1, 1)):
                        act(rdma(
                            src, HF.at[0, 1 - side], sHF.at[0, n], rHF.at[0, 1 - side],
                            (t, i + hop * (2 * side - 1)),
                        ))

        def prepare(start):
            for x in range(X):
                rock = IDW[start + x]
                v = looked_up(rock, 1)
                V[start + x] = v
                G[start + x] = 0.1 * looked_up(rock, 2)
                FE[0, start + x] = fraction(SB[0, start + x], v)

        def pair_copies():
            part = pl.ds(h * X, X)
            return (
                rdma(SB.at[0, part], SB.at[0, part], sA.at[0], rA.at[0], (t, pair)),
                rdma(IDW.at[part], IDW.at[part], sA.at[1], rA.at[1], (t, pair)),
            )

        for side in (0, 1):
            @pl.when(jnp.logical_not(side_here[side]))
            def _():
                def clear(r, c):
                    HF[r, side] = zero
                    return c

                lax.fori_loop(0, R, clear, 0)

        s0_in.wait()
        ids_win.wait()
        prepare(h * X)
        mult_in.wait()
        infl_in.wait()
        meet()
        send_fields()
        first_flow(lambda copy: copy.start())
        for d, peer in others_t:
            small_to(d, peer).start()
        rows = put_rows(u * XU, XU)
        pl.semaphore_wait(go, 1)
        for copy in pair_copies():
            copy.start()
        def sources(r):
            small_here(r)
            q_all = source(r, rows, XU)
            for x in range(XU):
                Q[x] = q_all[x]

        sources(0)
        there = pl.ds((1 - h) * X, X)
        rdma(SB.at[0, there], SB.at[0, there], sA.at[0], rA.at[0], (t, pair)).wait_recv()
        rdma(IDW.at[there], IDW.at[there], sA.at[1], rA.at[1], (t, pair)).wait_recv()
        prepare((1 - h) * X)

        def step(r, carry):
            for copy in handed(r):
                copy.wait_recv()
            for side in (0, 1):
                @pl.when(side_here[side])
                def _():
                    part = HF.at[r, side]
                    rdma(part, part, sHF.at[r, side], rHF.at[r, side], (t, pair)).wait_recv()

            def p_of(x):
                return PX[r, 0] if x < 0 else (PX[r, 1] if x >= XU else PB[r + 1, H + x])

            def f_of(x):
                return HF[r, 0] if x < 0 else (HF[r, 1] if x >= XU else FE[r, x])

            def face(ai, aj, pi, pj, fi, fj):
                fall = pi - pj
                return ai * aj * fall * jnp.where(fall > 0, fi, fj)

            def across(x):
                return face(SA[r, H + x - 1], SA[r, H + x], p_of(x - 1), p_of(x), f_of(x - 1), f_of(x))

            def transport(x, low, high):
                a = SA[r, H + x]
                p = p_of(x)
                f = f_of(x)
                s = SB[r, x]
                q = Q[x]
                cz = jnp.where(zi < Z - 1, face(a, after(a, 0), p, after(p, 0), f, after(f, 0)), 0.0)
                cy = jnp.where(yi < Y - 1, face(a, after(a, 1), p, after(p, 1), f, after(f, 1)), 0.0)
                out = (high - low) + (cz - before(cz, 0)) + (cy - before(cy, 1))
                gained = jnp.maximum(q, 0.0) * (1.0 - s) - jnp.maximum(-q, 0.0) * f - out
                s = s + G[x] * gained
                SB[r + 1, x] = s
                FE[r + 1, x] = fraction(s, V[x])

            for side in (0, 1):
                x = XU - 1 if side else 0
                transport(x, across(x), across(x + 1))

                @pl.when(jnp.logical_and(r < R - 1, side_here[side]))
                def _():
                    edge_flow(r + 1, side).start()

            low = across(1)
            for x in range(1, XU - 1):
                high = across(x + 1)
                transport(x, low, high)
                low = high
                if x == X - 1:
                    put_out(r, 0, SB.at[r + 1, pl.ds(0, X)], 1)
            put_out(r, 1, SB.at[r + 1, pl.ds(X, X)], 1)

            @pl.when(r < R - 1)
            def _():
                sources(r + 1)
            return carry

        lax.fori_loop(0, R, step, 0)
        misfit_here(False)
        outs_here()
        outs_sent(SB.at[0, pl.ds(0, X)], 1)
        for copy in pair_copies():
            copy.wait_send()

        first_flow(lambda copy: copy.wait_send())

        def done(r, c):
            for side in (0, 1):
                @pl.when(side_here[side])
                def _():
                    edge_flow(r, side).wait_send()
            return c

        lax.fori_loop(1, R, done, 0)

    each_field(lambda copy: copy.wait_send())
    for d, peer in others_t:
        small_to(d, peer).wait_send()


def deliver(mis_in, p_in, s_in, mis_out, p_out, s_out, row, done):
    members = p_in.shape[1]
    copies = []
    for n, (src, dst) in enumerate(((p_in, p_out), (s_in, s_out))):
        for m in range(members):
            copies.append(pltpu.make_async_copy(src.at[0, m], dst.at[0, m], done.at[n * members + m]))
    for copy in copies:
        copy.start()
    row[...] = mis_in[0, :members]
    last = pltpu.make_async_copy(row, mis_out, done.at[2 * members])
    last.start()
    for copy in copies + [last]:
        copy.wait()


def body(
    perm_field, step_multiplier, inflow, start_pressure, start_saturation,
    region_ids, region_table, well_cells, well_rates, observed,
):
    T = lax.axis_size("tm")
    N = lax.axis_size("space")
    X, Z, Y = start_pressure.shape
    W = well_cells.shape[0]
    members = perm_field.shape[0]
    assert members == T and T % 2 == 0 and N % 2 == 0 and X >= H and step_multiplier.shape[0] == 1
    assert Y & (Y - 1) == 0
    R = T
    U = N // 2
    XU = 2 * X
    WL = XU + 2 * H
    f32 = jnp.float32
    cell = (Z, Y)
    block = (X, Z, Y)
    window = (WL, Z, Y)
    unit = (XU, Z, Y)

    def buf(*shape):
        return pltpu.VMEM(shape, f32)

    dma = pltpu.SemaphoreType.DMA
    vmem = pl.BlockSpec(memory_space=pltpu.VMEM)
    anyspace = pl.BlockSpec(memory_space=pl.ANY)
    out_shape = jax.ShapeDtypeStruct((1, members) + block, f32)
    mis, outp, outs = pl.pallas_call(
        functools.partial(kernel, T, N),
        out_shape=(pltpu.VMEM((8, 128), f32), pltpu.VMEM(out_shape.shape, f32), pltpu.VMEM(out_shape.shape, f32)),
        in_specs=[anyspace] * 6 + [pl.BlockSpec(memory_space=pltpu.SMEM)] + [vmem] * 3,
        out_specs=(vmem, vmem, vmem),
        scratch_shapes=[
            buf(2, *block), pltpu.VMEM(block, jnp.int32), buf(R, *block), buf(R, *window), buf(*window),
            buf(R, *window), buf(R, *block), buf(R + 1, *window), buf(R, 2, *cell), buf(T, 8 * (T // 8 + 1), 128),
            buf(2, *window), buf(2, *window), buf(2, *window), buf(2, *window), buf(*window),
            buf(*window), buf(ITERS, *window),
            pltpu.VMEM(unit, jnp.int32), buf(R + 1, *unit), buf(R + 1, *unit), buf(R, 2, *cell),
            buf(*unit), buf(*unit), buf(*unit), buf(W, 1), buf(8, 128), buf(U, 8, 128), buf(T, 8, 128),
            dma((5,)), dma((2, T // 2)), dma((2, T)), dma((2 * R + 2, 3)), dma((2 * R + 2, 3)),
            dma((R, 3)), dma((R, 3)), dma((R + 1, 2)), dma((R + 1, 2)), dma((T,)), dma((T,)),
            dma((2,)), dma((2,)), dma((R, 2)), dma((R, 2)),
            dma((R, 2)), dma((2, T)), dma(()), dma((max(U, 2),)), dma((U,)), dma((2 * T - 1,)), dma((T,)),
            pltpu.SemaphoreType.REGULAR,
        ],
        compiler_params=pltpu.CompilerParams(
            has_side_effects=True, collective_id=0, vmem_limit_bytes=44 * 1024 * 1024
        ),
    )(
        perm_field, step_multiplier, inflow, start_pressure, start_saturation, region_ids,
        region_table, well_cells[None], well_rates, observed[:, 0, :],
    )
    return pl.pallas_call(
        deliver,
        out_shape=(jax.ShapeDtypeStruct((members,), f32), out_shape, out_shape),
        in_specs=[vmem, vmem, vmem],
        out_specs=(anyspace, anyspace, anyspace),
        scratch_shapes=[buf(members), dma((2 * members + 1,))],
    )(
        pltpu.with_memory_space_constraint(mis, pltpu.VMEM),
        pltpu.with_memory_space_constraint(outp, pltpu.VMEM),
        pltpu.with_memory_space_constraint(outs, pltpu.VMEM),
    )


def solution(mesh):
    return jax.shard_map(
        body,
        mesh=mesh,
        in_specs=(
            P(None, "space", None, None),
            P("tm", "space", None, None),
            P("tm", "space", None, None),
            P("space", None, None),
            P("space", None, None),
            P("space", None, None),
            P(),
            P(),
            P("tm", None),
            P(None, "tm", None),
        ),
        out_specs=(P(), P("tm", None, "space", None, None), P("tm", None, "space", None, None)),
        check_vma=False,
    )
```

```python
import functools

import jax
import jax.numpy as jnp
from jax import lax
from jax.experimental import pallas as pl
from jax.experimental.pallas import tpu as pltpu
from jax.sharding import PartitionSpec as P

ITERS = 3
H = ITERS + 1
MESH = pl.DeviceIdType.MESH
EXACT = lax.Precision.HIGHEST


def before(v, axis):
    return pltpu.roll(v, 1, axis)


def after(v, axis):
    return pltpu.roll(v, v.shape[axis] - 1, axis)


def kernel(
    T, N,
    perm, mult, infl, p0, s0, ids, table, cells, rates, seen_in,
    mis, outp, outs,
    PM, IDS, MS, IW, CW, SA, SO, PB, PX, SM, RC, SS, EE, QI, BB, DD, WW,
    IDW, SB, FE, HF, V, G, Q, ES, E0, E1, E2,
    lIN, sF, rF, sS, rS, sX, rX, sP, rP, sM, rM, sA, rA, sHF, rHF, sO, rO, lO, s1, r1, s2, r2, go,
):
    t = lax.axis_index("tm")
    i = lax.axis_index("space")
    X, Z, Y = IDS.shape
    R = T
    W = cells.shape[1]
    U = N // 2
    XU = 2 * X
    WL = XU + 2 * H
    row = t // 2
    core = lax.rem(t, 2)
    u = i // 2
    h = lax.rem(i, 2)
    mate = t + 1 - 2 * core
    pair = i + 1 - 2 * h
    member = 2 * row + h
    own = H + h * X
    side_here = (u > 0, u < U - 1)

    def load(n, src, dst):
        return pltpu.make_async_copy(src, dst, lIN.at[n])

    def rdma(src, dst, ss, rs, dev):
        return pltpu.make_async_remote_copy(
            src_ref=src, dst_ref=dst, send_sem=ss, recv_sem=rs, device_id=dev, device_id_type=MESH
        )

    mult_in = load(0, mult.at[0], MS.at[t])
    infl_in = load(1, infl.at[0], IW.at[t, pl.ds(own, X)])
    ids_in = load(2, ids, IDS)
    perm_in = load(3, perm.at[pl.ds(2 * row, 2)], PM)
    p0_in = load(4, p0, PB.at[0, pl.ds(own, X)])
    s0_in = load(3, s0, SB.at[0, pl.ds(h * X, X)])
    ids_win = load(4, ids, IDW.at[pl.ds(h * X, X)])
    mult_in.start()
    infl_in.start()

    @pl.when(core == 1)
    def _():
        perm_in.start()
        p0_in.start()
        ids_in.start()

    @pl.when(core == 0)
    def _():
        s0_in.start()
        ids_win.start()

    barrier = pltpu.get_barrier_semaphore()

    def greet(device):
        pl.semaphore_signal(barrier, inc=1, device_id=device, device_id_type=MESH)

    for d in range(1, T):
        peer = lax.rem(t + d, T)
        greet((peer, i))
        greet((peer, pair))
    for d in range(1, N):
        greet((t, lax.rem(i + d, N)))

    zi = lax.broadcasted_iota(jnp.int32, (Z, Y), 0)
    yi = lax.broadcasted_iota(jnp.int32, (Z, Y), 1)
    zero = jnp.zeros((Z, Y), jnp.float32)

    def neighbours(at, x):
        w = at(x)
        total = at(x - 1) + at(x + 1)
        total = total + (
            jnp.where(zi < Z - 1, after(w, 0), 0.0) + jnp.where(zi > 0, before(w, 0), 0.0)
        )
        return total + (
            jnp.where(yi < Y - 1, after(w, 1), 0.0) + jnp.where(yi > 0, before(w, 1), 0.0)
        )

    def looked_up(rock, which):
        v = zero
        for k in range(table.shape[1]):
            v = jnp.where(rock == k, table[which, k], v)
        return v

    def upright(line):
        eye = lax.broadcasted_iota(jnp.int32, (W, W), 0) == lax.broadcasted_iota(jnp.int32, (W, W), 1)
        return jnp.sum(jnp.where(eye, line, 0.0), axis=1, keepdims=True)

    bits = Y.bit_length() - 1
    rows_row = jnp.right_shift(cells[...], bits).astype(jnp.float32)
    cols_row = jnp.bitwise_and(cells[...], Y - 1).astype(jnp.float32)
    pick_cols = jnp.where(
        lax.broadcasted_iota(jnp.int32, (W, Y), 1).astype(jnp.float32) == upright(cols_row), 1.0, 0.0
    )
    SM[t] = jnp.zeros(SM.shape[1:], jnp.float32)
    SM[t, 0:1, 0:W] = rates[...]
    SM[t, 1:1 + T, 0:W] = seen_in[...]

    def put_rows(first, count):
        base = (first * Z).astype(jnp.float32)
        return jnp.where(
            lax.broadcasted_iota(jnp.int32, (count * Z, W), 0).astype(jnp.float32) == rows_row - base,
            1.0, 0.0,
        )

    others_t = [(d, lax.rem(t + d, T)) for d in range(1, T)]

    def small_to(d, peer):
        return rdma(SM.at[t], SM.at[t], sM.at[d], rM.at[t], (peer, i))

    def small_here(r):
        @pl.when(r != t)
        def _():
            rdma(SM.at[r], SM.at[r], sM.at[1], rM.at[r], (r, i)).wait_recv()

    def source(r, rows, count):
        rate = upright(SM[r, 0:1, 0:W])
        return jnp.dot(rows, pick_cols * rate, precision=EXACT).reshape(count, Z, Y)

    def field_to(rr):
        dev = (2 * rr + 1, i)
        return (
            rdma(MS.at[t], MS.at[t], sF.at[0, rr], rF.at[0, t], dev),
            rdma(
                IW.at[t, pl.ds(own, X)], IW.at[t, pl.ds(own, X)], sF.at[1, rr], rF.at[1, t], dev
            ),
        )

    def each_field(act):
        for rr in range(T // 2):
            @pl.when(t != 2 * rr + 1)
            def _():
                for copy in field_to(rr):
                    act(copy)

    def send_fields():
        each_field(lambda copy: copy.start())

    def put_out(r, half, src, which):
        dst = (outp, outs)[which].at[0, member]
        here = jnp.logical_and(r == t, half == h)

        @pl.when(jnp.logical_not(here))
        def _():
            rdma(src, dst, sO.at[r, half], rO.at[which, member], (r, 2 * u + half)).start()

        @pl.when(here)
        def _():
            pltpu.make_async_copy(src, dst, lO).start()

    def outs_sent(src, which):
        def sent(r, c):
            for half in (0, 1):
                dst = (outp, outs)[which].at[0, member]
                here = jnp.logical_and(r == t, half == h)

                @pl.when(jnp.logical_not(here))
                def _():
                    rdma(src, dst, sO.at[r, half], rO.at[which, member], (r, 2 * u + half)).wait_send()
            return c

        lax.fori_loop(0, R, sent, 0)
        pltpu.make_async_copy(src, (outp, outs)[which].at[0, member], lO).wait()

    def outs_here():
        for which in (0, 1):
            for m in range(T):
                mine = jnp.logical_and(core == 1 - which, m == member)

                @pl.when(jnp.logical_not(mine))
                def _():
                    dst = (outp, outs)[which].at[0, m]
                    rdma(dst, dst, sO.at[0, 0], rO.at[which, m], (t, pair)).wait_recv()

    def misfit_here(skip):
        for m in range(T):
            wait = rdma(E2.at[m], E2.at[m], s2.at[0], r2.at[m], (t, pair))
            if skip:
                @pl.when(m != member)
                def _():
                    wait.wait_recv()
            else:
                wait.wait_recv()
        lanes = lax.broadcasted_iota(jnp.int32, (8, 128), 1)
        result = jnp.zeros((8, 128), jnp.float32)
        for m in range(T):
            result = result + jnp.where(lanes == m, E2[m], 0.0)
        mis[...] = result * (1.0 / (R * W))

    def edge_of(side, depth):
        src = pl.ds(H + XU - depth if side else H, depth)
        dst = pl.ds(H - depth if side else H + XU, depth)
        return src, dst

    def pooled(n, window, other):
        return rdma(
            other.at[pl.ds(0, X)], window.at[pl.ds(own, X)], sS.at[n, 0], rS.at[n, 0], (t, pair)
        )

    def halo(n, window, depth, side, relayed):
        src, dst = edge_of(side, depth)
        return rdma(
            window.at[src], window.at[dst], sS.at[n, 1 + relayed], rS.at[n, 2 - side],
            (t, i + 4 * side - 2),
        )

    def halos(n, window, depth, relayed, act):
        for side in (0, 1):
            @pl.when(jnp.logical_and(side_here[side], h == (1 - side if relayed else side)))
            def _():
                act(halo(n, window, depth, side, relayed))

    def pool(n, window, depth, other):
        pooled(n, window, other).start()
        halos(n, window, depth, 0, lambda copy: copy.start())

    def relay(n, window, depth, other):
        part = window.at[pl.ds(H + (1 - h) * X, X)]
        rdma(part, part, sS.at[n, 0], rS.at[n, 0], (t, pair)).wait_recv()
        halos(n, window, depth, 1, lambda copy: copy.start())

    def spread_here(n, window, depth, other):
        for side in (0, 1):
            @pl.when(side_here[side])
            def _():
                part = window.at[pl.ds(H + XU if side else H - depth, depth)]
                rdma(part, part, sS.at[n, 1], rS.at[n, 1 + side], (t, pair)).wait_recv()

    def spread_sent(n, window, depth, other):
        pooled(n, window, other).wait_send()
        for relayed in (0, 1):
            halos(n, window, depth, relayed, lambda copy: copy.wait_send())

    def own_of(window):
        return window.at[pl.ds(own, X)]

    def conduct_args(r):
        return r, SA.at[r], H, SO.at[r]

    def inflow_args(r):
        return R + r, IW.at[r], H - 1, own_of(IW.at[r])

    def pressure_args():
        return 2 * R, PB.at[0], H, own_of(PB.at[0])

    def storage_args():
        return 2 * R + 1, CW, H - 1, own_of(CW)

    def distribute(r):
        @pl.when(r != t)
        def _():
            rdma(MS.at[r], MS.at[r], sF.at[0, 0], rF.at[0, r], (r, i)).wait_recv()

        for x in range(X):
            SO[r, x] = jnp.sqrt(PM[1 - h, x] * MS[r, x])
            SA[r, own + x] = jnp.sqrt(PM[h, x] * MS[r, x])
        pool(*conduct_args(r))

        @pl.when(r != t)
        def _():
            mine = own_of(IW.at[r])
            rdma(mine, mine, sF.at[1, 0], rF.at[1, r], (r, i)).wait_recv()
        pool(*inflow_args(r))

    def round_of(k, side):
        if side == 0:
            src, dst, dev = pl.ds(H, H), pl.ds(H + XU, H), (t, i - 2)
        else:
            src, dst, dev = pl.ds(XU, H), pl.ds(0, H), (t, i + 2)
        return rdma(PB.at[k, src], PB.at[k, dst], sP.at[k, side], rP.at[k, 1 - side], dev)

    def handed(r):
        mid = pl.ds(H, XU)
        wide = pl.ds(H - 1, XU + 2)
        dev = (mate, i)
        return (
            rdma(SA.at[r, wide], SA.at[r, wide], sX.at[r, 0], rX.at[r, 0], dev),
            rdma(PB.at[r + 1, mid], PB.at[r + 1, mid], sX.at[r, 1], rX.at[r, 1], dev),
            rdma(PX.at[r], PX.at[r], sX.at[r, 2], rX.at[r, 2], dev),
        )

    def meet():
        pl.semaphore_wait(barrier, (N - 1) + 2 * (T - 1))

    @pl.when(core == 1)
    def _():
        ids_in.wait()
        for x in range(X):
            CW[own + x] = looked_up(IDS[x], 0)
        for side in (0, 1):
            @pl.when(jnp.logical_not(side_here[side]))
            def _():
                first = H + XU if side else 0
                for x in range(first, first + H):
                    CW[x] = zero + 1.0

                def clear(r, c):
                    for x in range(first, first + H):
                        SA[r, x] = zero
                        IW[r, x] = zero
                        PB[r, x] = zero
                    return c

                lax.fori_loop(0, R, clear, 0)
        p0_in.wait()
        mult_in.wait()
        infl_in.wait()
        perm_in.wait()
        meet()
        pool(*pressure_args())
        pool(*storage_args())
        for d, peer in others_t:
            small_to(d, peer).start()
        distribute(0)
        pl.semaphore_signal(go, inc=1, device_id=(mate, i), device_id_type=MESH)
        send_fields()
        rows = put_rows(u * XU - H, WL)
        local = upright(rows_row) - (u * (XU * Z)).astype(jnp.float32)
        pick_rows = jnp.where(
            lax.broadcasted_iota(jnp.int32, (W, XU * Z), 1).astype(jnp.float32) == local, 1.0, 0.0
        )
        owned = jnp.sum(pick_rows, axis=1, keepdims=True)
        ES[...] = jnp.zeros(ES.shape, jnp.float32)

        def coefficients(r):
            slot = lax.rem(r, 2)
            spread_here(*conduct_args(r))
            handed(r)[0].start()
            for x in range(1, WL - 1):
                a = SA[r, x]
                rc = 1.0 / (CW[x] + a * neighbours(lambda y: SA[r, y], x))
                RC[slot, x] = rc
                ss = a * rc
                SS[slot, x] = ss
                EE[slot, x] = a * ss
            small_here(r)
            q = source(r, rows, WL)
            spread_here(*inflow_args(r))
            for x in range(1, WL - 1):
                QI[slot, x] = q[x] + IW[r, x]

        def relay_fields(r):
            relay(*conduct_args(r))
            relay(*inflow_args(r))

        relay(*pressure_args())
        relay(*storage_args())
        relay_fields(0)
        distribute(1)
        if R > 2:
            distribute(2)
        spread_here(*pressure_args())
        spread_here(*storage_args())
        coefficients(0)
        relay_fields(1)

        def step(r, carry):
            slot = lax.rem(r, 2)

            def first(layers):
                for x in layers:
                    WW[0, x] = SA[r, x] * PB[r, x]

            def sweep_one(layers):
                for x in layers:
                    b = CW[x] * PB[r, x] + QI[slot, x]
                    d = SS[slot, x] * b
                    BB[x] = b
                    DD[x] = d
                    WW[1, x] = d + EE[slot, x] * neighbours(lambda y: WW[0, y], x)

            first(range(H, H + XU))
            sweep_one(range(H + 1, H + XU - 1))

            @pl.when(r > 0)
            def _():
                for side in (0, 1):
                    @pl.when(side_here[side])
                    def _():
                        part = PB.at[r, pl.ds(H + XU if side else 0, H)]
                        rdma(part, part, sP.at[r, side], rP.at[r, side], (t, pair)).wait_recv()

            first(range(0, H))
            sweep_one(range(1, H + 1))
            first(range(H + XU, WL))
            sweep_one(range(H + XU - 1, WL - 1))
            for j in range(1, ITERS - 1):
                for x in range(j + 1, WL - j - 1):
                    WW[j + 1, x] = DD[x] + EE[slot, x] * neighbours(lambda y: WW[j, y], x)

            def last(x):
                return RC[slot, x] * (
                    BB[x] + SA[r, x] * neighbours(lambda y: WW[ITERS - 1, y], x)
                )

            def send(side):
                @pl.when(jnp.logical_and(r < R - 1, side_here[side]))
                def _():
                    round_of(r + 1, side).start()

            for x in range(H, H + X):
                PB[r + 1, x] = last(x)
            send(0)
            for x in range(H + X, H + XU):
                PB[r + 1, x] = last(x)
            send(1)
            handed(r)[1].start()
            for half in (0, 1):
                put_out(r, half, PB.at[r + 1, pl.ds(H + half * X, X)], 0)
            PX[r, 0] = last(H - 1)
            PX[r, 1] = last(H + XU)
            handed(r)[2].start()
            seen = jnp.dot(pick_rows, PB[r + 1, H:H + XU].reshape(XU * Z, Y), precision=EXACT)
            predicted = jnp.sum(seen * pick_cols, axis=1, keepdims=True)
            lines = lax.broadcasted_iota(jnp.int32, SM.shape[1:], 0)
            seen_row = jnp.sum(jnp.where(lines == 1 + member, SM[r], 0.0), axis=0, keepdims=True)
            gap = predicted - upright(seen_row[:, :W])
            ES[...] = ES[...] + owned * gap * gap

            @pl.when(r == R - 1)
            def _():
                E0[...] = jnp.broadcast_to(jnp.sum(ES[...], axis=0, keepdims=True), E0.shape)
                for d in range(1, U):
                    peer = lax.rem(u + d, U)
                    rdma(E0, E1.at[u], s1.at[d], r1.at[u], (t, 2 * peer + h)).start()

            @pl.when(r < R - 1)
            def _():
                coefficients(r + 1)

            @pl.when(r < R - 2)
            def _():
                relay_fields(r + 2)

            @pl.when(r < R - 3)
            def _():
                distribute(r + 3)
            return carry

        lax.fori_loop(0, R, step, 0)
        E1[u] = E0[...]
        for d in range(1, U):
            peer = lax.rem(u + d, U)
            rdma(E1.at[peer], E1.at[peer], s1.at[d], r1.at[peer], (t, pair)).wait_recv()
        whole = E1[0]
        for n in range(1, U):
            whole = whole + E1[n]
        E2[member] = whole

        def plane(act):
            n = 0
            for d in range(T):
                for half in (0, 1):
                    if d == 0 and half == 0:
                        continue
                    dev = (lax.rem(t + d, T), i if half == 0 else pair)
                    act(rdma(E2.at[member], E2.at[member], s2.at[n], r2.at[member], dev))
                    n += 1

        plane(lambda copy: copy.start())
        misfit_here(True)
        outs_here()
        outs_sent(PB.at[0, pl.ds(0, X)], 0)
        plane(lambda copy: copy.wait_send())
        for d in range(1, U):
            peer = lax.rem(u + d, U)
            rdma(E0, E1.at[u], s1.at[d], r1.at[u], (t, 2 * peer + h)).wait_send()

        def done(r, c):
            spread_sent(*conduct_args(r))
            spread_sent(*inflow_args(r))
            for copy in handed(r):
                copy.wait_send()

            @pl.when(r > 0)
            def _():
                for side in (0, 1):
                    @pl.when(side_here[side])
                    def _():
                        round_of(r, side).wait_send()
            return c

        lax.fori_loop(0, R, done, 0)
        spread_sent(*pressure_args())
        spread_sent(*storage_args())

    @pl.when(core == 0)
    def _():
        def fraction(s, v):
            sq = s * s
            rest = (1.0 - s) * (1.0 - s)
            return sq / (sq + v * rest)

        def edge_flow(r, side):
            src = FE.at[r, XU - 1 if side else 0]
            return rdma(
                src, HF.at[r, 1 - side], sHF.at[r, side], rHF.at[r, 1 - side], (t, i + 4 * side - 2)
            )

        def first_flow(act):
            for side in (0, 1):
                @pl.when(jnp.logical_and(side_here[side], h == side))
                def _():
                    src = FE.at[0, XU - 1 if side else 0]
                    for n, hop in ((0, 2), (1, 1)):
                        act(rdma(
                            src, HF.at[0, 1 - side], sHF.at[0, n], rHF.at[0, 1 - side],
                            (t, i + hop * (2 * side - 1)),
                        ))

        def prepare(start):
            for x in range(X):
                rock = IDW[start + x]
                v = looked_up(rock, 1)
                V[start + x] = v
                G[start + x] = 0.1 * looked_up(rock, 2)
                FE[0, start + x] = fraction(SB[0, start + x], v)

        def pair_copies():
            part = pl.ds(h * X, X)
            return (
                rdma(SB.at[0, part], SB.at[0, part], sA.at[0], rA.at[0], (t, pair)),
                rdma(IDW.at[part], IDW.at[part], sA.at[1], rA.at[1], (t, pair)),
            )

        for side in (0, 1):
            @pl.when(jnp.logical_not(side_here[side]))
            def _():
                def clear(r, c):
                    HF[r, side] = zero
                    return c

                lax.fori_loop(0, R, clear, 0)

        s0_in.wait()
        ids_win.wait()
        prepare(h * X)
        mult_in.wait()
        infl_in.wait()
        meet()
        send_fields()
        first_flow(lambda copy: copy.start())
        for d, peer in others_t:
            small_to(d, peer).start()
        rows = put_rows(u * XU, XU)
        pl.semaphore_wait(go, 1)
        for copy in pair_copies():
            copy.start()
        def sources(r):
            small_here(r)
            q_all = source(r, rows, XU)
            for x in range(XU):
                Q[x] = q_all[x]

        sources(0)
        there = pl.ds((1 - h) * X, X)
        rdma(SB.at[0, there], SB.at[0, there], sA.at[0], rA.at[0], (t, pair)).wait_recv()
        rdma(IDW.at[there], IDW.at[there], sA.at[1], rA.at[1], (t, pair)).wait_recv()
        prepare((1 - h) * X)

        def step(r, carry):
            for copy in handed(r):
                copy.wait_recv()
            for side in (0, 1):
                @pl.when(side_here[side])
                def _():
                    part = HF.at[r, side]
                    rdma(part, part, sHF.at[r, side], rHF.at[r, side], (t, pair)).wait_recv()

            def p_of(x):
                return PX[r, 0] if x < 0 else (PX[r, 1] if x >= XU else PB[r + 1, H + x])

            def f_of(x):
                return HF[r, 0] if x < 0 else (HF[r, 1] if x >= XU else FE[r, x])

            def face(ai, aj, pi, pj, fi, fj):
                fall = pi - pj
                return ai * aj * fall * jnp.where(fall > 0, fi, fj)

            def across(x):
                return face(SA[r, H + x - 1], SA[r, H + x], p_of(x - 1), p_of(x), f_of(x - 1), f_of(x))

            def transport(x, low, high):
                a = SA[r, H + x]
                p = p_of(x)
                f = f_of(x)
                s = SB[r, x]
                q = Q[x]
                cz = jnp.where(zi < Z - 1, face(a, after(a, 0), p, after(p, 0), f, after(f, 0)), 0.0)
                cy = jnp.where(yi < Y - 1, face(a, after(a, 1), p, after(p, 1), f, after(f, 1)), 0.0)
                out = (high - low) + (cz - before(cz, 0)) + (cy - before(cy, 1))
                gained = jnp.maximum(q, 0.0) * (1.0 - s) - jnp.maximum(-q, 0.0) * f - out
                s = s + G[x] * gained
                SB[r + 1, x] = s
                FE[r + 1, x] = fraction(s, V[x])

            for side in (0, 1):
                x = XU - 1 if side else 0
                transport(x, across(x), across(x + 1))

                @pl.when(jnp.logical_and(r < R - 1, side_here[side]))
                def _():
                    edge_flow(r + 1, side).start()

            low = across(1)
            for x in range(1, XU - 1):
                high = across(x + 1)
                transport(x, low, high)
                low = high
                if x == X - 1:
                    put_out(r, 0, SB.at[r + 1, pl.ds(0, X)], 1)
            put_out(r, 1, SB.at[r + 1, pl.ds(X, X)], 1)

            @pl.when(r < R - 1)
            def _():
                sources(r + 1)
            return carry

        lax.fori_loop(0, R, step, 0)
        misfit_here(False)
        outs_here()
        outs_sent(SB.at[0, pl.ds(0, X)], 1)
        for copy in pair_copies():
            copy.wait_send()

        first_flow(lambda copy: copy.wait_send())

        def done(r, c):
            for side in (0, 1):
                @pl.when(side_here[side])
                def _():
                    edge_flow(r, side).wait_send()
            return c

        lax.fori_loop(1, R, done, 0)

    each_field(lambda copy: copy.wait_send())
    for d, peer in others_t:
        small_to(d, peer).wait_send()


def deliver(mis_in, p_in, s_in, mis_out, p_out, s_out, row, done):
    members = p_in.shape[1]
    copies = []
    for n, (src, dst) in enumerate(((p_in, p_out), (s_in, s_out))):
        for m in range(members):
            copies.append(pltpu.make_async_copy(src.at[0, m], dst.at[0, m], done.at[n * members + m]))
    for copy in copies:
        copy.start()
    row[...] = mis_in[0, :members]
    last = pltpu.make_async_copy(row, mis_out, done.at[2 * members])
    last.start()
    for copy in copies + [last]:
        copy.wait()


def body(
    perm_field, step_multiplier, inflow, start_pressure, start_saturation,
    region_ids, region_table, well_cells, well_rates, observed,
):
    T = lax.axis_size("tm")
    N = lax.axis_size("space")
    X, Z, Y = start_pressure.shape
    W = well_cells.shape[0]
    members = perm_field.shape[0]
    assert members == T and T % 2 == 0 and N % 2 == 0 and X >= H and step_multiplier.shape[0] == 1
    assert Y & (Y - 1) == 0
    R = T
    U = N // 2
    XU = 2 * X
    WL = XU + 2 * H
    f32 = jnp.float32
    cell = (Z, Y)
    block = (X, Z, Y)
    window = (WL, Z, Y)
    unit = (XU, Z, Y)

    def buf(*shape):
        return pltpu.VMEM(shape, f32)

    dma = pltpu.SemaphoreType.DMA
    vmem = pl.BlockSpec(memory_space=pltpu.VMEM)
    anyspace = pl.BlockSpec(memory_space=pl.ANY)
    out_shape = jax.ShapeDtypeStruct((1, members) + block, f32)
    mis, outp, outs = pl.pallas_call(
        functools.partial(kernel, T, N),
        out_shape=(pltpu.VMEM((8, 128), f32), pltpu.VMEM(out_shape.shape, f32), pltpu.VMEM(out_shape.shape, f32)),
        in_specs=[pl.BlockSpec(memory_space=pltpu.HBM)] * 6 + [pl.BlockSpec(memory_space=pltpu.SMEM)] + [vmem] * 3,
        out_specs=(vmem, vmem, vmem),
        scratch_shapes=[
            buf(2, *block), pltpu.VMEM(block, jnp.int32), buf(R, *block), buf(R, *window), buf(*window),
            buf(R, *window), buf(R, *block), buf(R + 1, *window), buf(R, 2, *cell), buf(T, 8 * (T // 8 + 1), 128),
            buf(2, *window), buf(2, *window), buf(2, *window), buf(2, *window), buf(*window),
            buf(*window), buf(ITERS, *window),
            pltpu.VMEM(unit, jnp.int32), buf(R + 1, *unit), buf(R + 1, *unit), buf(R, 2, *cell),
            buf(*unit), buf(*unit), buf(*unit), buf(W, 1), buf(8, 128), buf(U, 8, 128), buf(T, 8, 128),
            dma((5,)), dma((2, T // 2)), dma((2, T)), dma((2 * R + 2, 3)), dma((2 * R + 2, 3)),
            dma((R, 3)), dma((R, 3)), dma((R + 1, 2)), dma((R + 1, 2)), dma((T,)), dma((T,)),
            dma((2,)), dma((2,)), dma((R, 2)), dma((R, 2)),
            dma((R, 2)), dma((2, T)), dma(()), dma((max(U, 2),)), dma((U,)), dma((2 * T - 1,)), dma((T,)),
            pltpu.SemaphoreType.REGULAR,
        ],
        compiler_params=pltpu.CompilerParams(
            has_side_effects=True, collective_id=0, vmem_limit_bytes=56 * 1024 * 1024
        ),
    )(
        perm_field, step_multiplier, inflow, start_pressure, start_saturation, region_ids,
        region_table, well_cells[None], well_rates, observed[:, 0, :],
    )
    return pl.pallas_call(
        deliver,
        out_shape=(jax.ShapeDtypeStruct((members,), f32), out_shape, out_shape),
        in_specs=[vmem, vmem, vmem],
        out_specs=(anyspace, anyspace, anyspace),
        scratch_shapes=[buf(members), dma((2 * members + 1,))],
    )(
        pltpu.with_memory_space_constraint(mis, pltpu.VMEM),
        pltpu.with_memory_space_constraint(outp, pltpu.VMEM),
        pltpu.with_memory_space_constraint(outs, pltpu.VMEM),
    )


def solution(mesh):
    return jax.shard_map(
        body,
        mesh=mesh,
        in_specs=(
            P(None, "space", None, None),
            P("tm", "space", None, None),
            P("tm", "space", None, None),
            P("space", None, None),
            P("space", None, None),
            P("space", None, None),
            P(),
            P(),
            P("tm", None),
            P(None, "tm", None),
        ),
        out_specs=(P(), P("tm", None, "space", None, None), P("tm", None, "space", None, None)),
        check_vma=False,
    )
```

```python
import functools

import jax
import jax.numpy as jnp
from jax import lax
from jax.experimental import pallas as pl
from jax.experimental.pallas import tpu as pltpu
from jax.sharding import PartitionSpec as P

ITERS = 3
H = ITERS + 1
MESH = pl.DeviceIdType.MESH
EXACT = lax.Precision.HIGHEST


def before(v, axis):
    return pltpu.roll(v, 1, axis)


def after(v, axis):
    return pltpu.roll(v, v.shape[axis] - 1, axis)


def kernel(
    T, N,
    perm, mult, infl, p0, s0, ids, table, cells, rates, seen_in,
    mis, outp, outs,
    PM, IR, MS, IW, CW, SA, SO, PB, PX, SM, RC, SS, EE, QI, BB, DD, WW,
    IDW, SB, FE, HF, V, G, Q, ES, E0, E1, E2,
    lIN, sF, rF, sS, rS, sX, rX, sP, rP, sM, rM, sA, rA, sHF, rHF, sO, rO, lO, s1, r1, s2, r2, go,
):
    t = lax.axis_index("tm")
    i = lax.axis_index("space")
    X, Z, Y = p0.shape
    R = T
    W = cells.shape[1]
    U = N // 2
    XU = 2 * X
    WL = XU + 2 * H
    row = t // 2
    core = lax.rem(t, 2)
    u = i // 2
    h = lax.rem(i, 2)
    mate = t + 1 - 2 * core
    pair = i + 1 - 2 * h
    member = 2 * row + h
    own = H + h * X
    side_here = (u > 0, u < U - 1)

    def load(n, src, dst):
        return pltpu.make_async_copy(src, dst, lIN.at[n])

    def rdma(src, dst, ss, rs, dev):
        return pltpu.make_async_remote_copy(
            src_ref=src, dst_ref=dst, send_sem=ss, recv_sem=rs, device_id=dev, device_id_type=MESH
        )

    mult_in = load(0, mult.at[0], MS.at[t])
    infl_in = load(1, infl.at[0], IW.at[t, pl.ds(own, X)])
    ids_in = load(2, ids, IR.at[pl.ds(own, X)])
    perm_in = load(3, perm.at[pl.ds(2 * row, 2)], PM)
    p0_in = load(4, p0, PB.at[0, pl.ds(own, X)])
    s0_in = load(3, s0, SB.at[0, pl.ds(h * X, X)])
    ids_win = load(4, ids, IDW.at[pl.ds(h * X, X)])
    mult_in.start()
    infl_in.start()

    @pl.when(core == 1)
    def _():
        perm_in.start()
        p0_in.start()
        ids_in.start()

    @pl.when(core == 0)
    def _():
        s0_in.start()
        ids_win.start()

    barrier = pltpu.get_barrier_semaphore()

    def greet(device):
        pl.semaphore_signal(barrier, inc=1, device_id=device, device_id_type=MESH)

    for d in range(1, T):
        peer = lax.rem(t + d, T)
        greet((peer, i))
        greet((peer, pair))
    for d in range(1, N):
        greet((t, lax.rem(i + d, N)))

    zi = lax.broadcasted_iota(jnp.int32, (Z, Y), 0)
    yi = lax.broadcasted_iota(jnp.int32, (Z, Y), 1)
    zero = jnp.zeros((Z, Y), jnp.float32)

    def neighbours(at, x):
        w = at(x)
        total = at(x - 1) + at(x + 1)
        total = total + (
            jnp.where(zi < Z - 1, after(w, 0), 0.0) + jnp.where(zi > 0, before(w, 0), 0.0)
        )
        return total + (
            jnp.where(yi < Y - 1, after(w, 1), 0.0) + jnp.where(yi > 0, before(w, 1), 0.0)
        )

    def looked_up(rock, which):
        v = zero
        for k in range(table.shape[1]):
            v = jnp.where(rock == k, table[which, k], v)
        return v

    def upright(line):
        eye = lax.broadcasted_iota(jnp.int32, (W, W), 0) == lax.broadcasted_iota(jnp.int32, (W, W), 1)
        return jnp.sum(jnp.where(eye, line, 0.0), axis=1, keepdims=True)

    bits = Y.bit_length() - 1
    rows_row = jnp.right_shift(cells[...], bits).astype(jnp.float32)
    cols_row = jnp.bitwise_and(cells[...], Y - 1).astype(jnp.float32)
    pick_cols = jnp.where(
        lax.broadcasted_iota(jnp.int32, (W, Y), 1).astype(jnp.float32) == upright(cols_row), 1.0, 0.0
    )
    SM[t] = jnp.zeros(SM.shape[1:], jnp.float32)
    SM[t, 0:1, 0:W] = rates[...]
    SM[t, 1:1 + T, 0:W] = seen_in[...]

    def put_rows(first, count):
        base = (first * Z).astype(jnp.float32)
        return jnp.where(
            lax.broadcasted_iota(jnp.int32, (count * Z, W), 0).astype(jnp.float32) == rows_row - base,
            1.0, 0.0,
        )

    others_t = [(d, lax.rem(t + d, T)) for d in range(1, T)]

    def small_to(d, peer):
        return rdma(SM.at[t], SM.at[t], sM.at[d], rM.at[t], (peer, i))

    def small_here(r):
        @pl.when(r != t)
        def _():
            rdma(SM.at[r], SM.at[r], sM.at[1], rM.at[r], (r, i)).wait_recv()

    def source(r, rows, count):
        rate = upright(SM[r, 0:1, 0:W])
        return jnp.dot(rows, pick_cols * rate, precision=EXACT).reshape(count, Z, Y)

    def field_to(rr):
        dev = (2 * rr + 1, i)
        return (
            rdma(MS.at[t], MS.at[t], sF.at[0, rr], rF.at[0, t], dev),
            rdma(
                IW.at[t, pl.ds(own, X)], IW.at[t, pl.ds(own, X)], sF.at[1, rr], rF.at[1, t], dev
            ),
        )

    def each_field(act):
        for rr in range(T // 2):
            @pl.when(t != 2 * rr + 1)
            def _():
                for copy in field_to(rr):
                    act(copy)

    def send_fields():
        each_field(lambda copy: copy.start())

    def put_out(r, half, src, which):
        dst = (outp, outs)[which].at[0, member]
        here = jnp.logical_and(r == t, half == h)

        @pl.when(jnp.logical_not(here))
        def _():
            rdma(src, dst, sO.at[r, half], rO.at[which, member], (r, 2 * u + half)).start()

        @pl.when(here)
        def _():
            pltpu.make_async_copy(src, dst, lO).start()

    def outs_sent(src, which):
        def sent(r, c):
            for half in (0, 1):
                dst = (outp, outs)[which].at[0, member]
                here = jnp.logical_and(r == t, half == h)

                @pl.when(jnp.logical_not(here))
                def _():
                    rdma(src, dst, sO.at[r, half], rO.at[which, member], (r, 2 * u + half)).wait_send()
            return c

        lax.fori_loop(0, R, sent, 0)
        pltpu.make_async_copy(src, (outp, outs)[which].at[0, member], lO).wait()

    def outs_here():
        for which in (0, 1):
            for m in range(T):
                mine = jnp.logical_and(core == 1 - which, m == member)

                @pl.when(jnp.logical_not(mine))
                def _():
                    dst = (outp, outs)[which].at[0, m]
                    rdma(dst, dst, sO.at[0, 0], rO.at[which, m], (t, pair)).wait_recv()

    def misfit_here(skip):
        for m in range(T):
            wait = rdma(E2.at[m], E2.at[m], s2.at[0], r2.at[m], (t, pair))
            if skip:
                @pl.when(m != member)
                def _():
                    wait.wait_recv()
            else:
                wait.wait_recv()
        lanes = lax.broadcasted_iota(jnp.int32, (8, 128), 1)
        result = jnp.zeros((8, 128), jnp.float32)
        for m in range(T):
            result = result + jnp.where(lanes == m, E2[m], 0.0)
        mis[...] = result * (1.0 / (R * W))

    def edge_of(side, depth):
        src = pl.ds(H + XU - depth if side else H, depth)
        dst = pl.ds(H - depth if side else H + XU, depth)
        return src, dst

    def pooled(n, window, other):
        return rdma(
            other.at[pl.ds(0, X)], window.at[pl.ds(own, X)], sS.at[n, 0], rS.at[n, 0], (t, pair)
        )

    def halo(n, window, depth, side, relayed):
        src, dst = edge_of(side, depth)
        return rdma(
            window.at[src], window.at[dst], sS.at[n, 1 + relayed], rS.at[n, 2 - side],
            (t, i + 4 * side - 2),
        )

    def halos(n, window, depth, relayed, act):
        for side in (0, 1):
            @pl.when(jnp.logical_and(side_here[side], h == (1 - side if relayed else side)))
            def _():
                act(halo(n, window, depth, side, relayed))

    def pool(n, window, depth, other):
        pooled(n, window, other).start()
        halos(n, window, depth, 0, lambda copy: copy.start())

    def relay(n, window, depth, other):
        part = window.at[pl.ds(H + (1 - h) * X, X)]
        rdma(part, part, sS.at[n, 0], rS.at[n, 0], (t, pair)).wait_recv()
        halos(n, window, depth, 1, lambda copy: copy.start())

    def spread_here(n, window, depth, other):
        for side in (0, 1):
            @pl.when(side_here[side])
            def _():
                part = window.at[pl.ds(H + XU if side else H - depth, depth)]
                rdma(part, part, sS.at[n, 1], rS.at[n, 1 + side], (t, pair)).wait_recv()

    def spread_sent(n, window, depth, other):
        pooled(n, window, other).wait_send()
        for relayed in (0, 1):
            halos(n, window, depth, relayed, lambda copy: copy.wait_send())

    def own_of(window):
        return window.at[pl.ds(own, X)]

    def conduct_args(r):
        return r, SA.at[r], H, SO.at[r]

    def inflow_args(r):
        return R + r, IW.at[r], H - 1, own_of(IW.at[r])

    def pressure_args():
        return 2 * R, PB.at[0], H, own_of(PB.at[0])

    def storage_args():
        return 2 * R + 1, IR, H - 1, own_of(IR)

    def distribute(r):
        @pl.when(r != t)
        def _():
            rdma(MS.at[r], MS.at[r], sF.at[0, 0], rF.at[0, r], (r, i)).wait_recv()

        for x in range(X):
            SO[r, x] = jnp.sqrt(PM[1 - h, x] * MS[r, x])
            SA[r, own + x] = jnp.sqrt(PM[h, x] * MS[r, x])
        pool(*conduct_args(r))

        @pl.when(r != t)
        def _():
            mine = own_of(IW.at[r])
            rdma(mine, mine, sF.at[1, 0], rF.at[1, r], (r, i)).wait_recv()
        pool(*inflow_args(r))

    def round_of(k, side):
        if side == 0:
            src, dst, dev = pl.ds(H, H), pl.ds(H + XU, H), (t, i - 2)
        else:
            src, dst, dev = pl.ds(XU, H), pl.ds(0, H), (t, i + 2)
        return rdma(PB.at[k, src], PB.at[k, dst], sP.at[k, side], rP.at[k, 1 - side], dev)

    def handed(r):
        mid = pl.ds(H, XU)
        wide = pl.ds(H - 1, XU + 2)
        dev = (mate, i)
        return (
            rdma(SA.at[r, wide], SA.at[r, wide], sX.at[r, 0], rX.at[r, 0], dev),
            rdma(PB.at[r + 1, mid], PB.at[r + 1, mid], sX.at[r, 1], rX.at[r, 1], dev),
            rdma(PX.at[r], PX.at[r], sX.at[r, 2], rX.at[r, 2], dev),
        )

    def ids_handed():
        return rdma(
            IR.at[pl.ds(H + (1 - h) * X, X)], IDW.at[pl.ds((1 - h) * X, X)], sA.at[1], rA.at[1], (mate, i)
        )

    def meet():
        pl.semaphore_wait(barrier, (N - 1) + 2 * (T - 1))

    @pl.when(core == 1)
    def _():
        ids_in.wait()
        for x in range(X):
            CW[own + x] = looked_up(IR[own + x], 0)
        for side in (0, 1):
            @pl.when(jnp.logical_not(side_here[side]))
            def _():
                first = H + XU if side else 0
                for x in range(first, first + H):
                    CW[x] = zero + 1.0

                def clear(r, c):
                    for x in range(first, first + H):
                        SA[r, x] = zero
                        IW[r, x] = zero
                        PB[r, x] = zero
                    return c

                lax.fori_loop(0, R, clear, 0)
        p0_in.wait()
        mult_in.wait()
        infl_in.wait()
        perm_in.wait()
        meet()
        pool(*pressure_args())
        pool(*storage_args())
        for d, peer in others_t:
            small_to(d, peer).start()
        distribute(0)
        pl.semaphore_signal(go, inc=1, device_id=(mate, i), device_id_type=MESH)
        send_fields()
        rows = put_rows(u * XU - H, WL)
        local = upright(rows_row) - (u * (XU * Z)).astype(jnp.float32)
        pick_rows = jnp.where(
            lax.broadcasted_iota(jnp.int32, (W, XU * Z), 1).astype(jnp.float32) == local, 1.0, 0.0
        )
        owned = jnp.sum(pick_rows, axis=1, keepdims=True)
        ES[...] = jnp.zeros(ES.shape, jnp.float32)

        def coefficients(r):
            slot = lax.rem(r, 2)
            spread_here(*conduct_args(r))
            handed(r)[0].start()
            for x in range(1, WL - 1):
                a = SA[r, x]
                rc = 1.0 / (CW[x] + a * neighbours(lambda y: SA[r, y], x))
                RC[slot, x] = rc
                ss = a * rc
                SS[slot, x] = ss
                EE[slot, x] = a * ss
            small_here(r)
            q = source(r, rows, WL)
            spread_here(*inflow_args(r))
            for x in range(1, WL - 1):
                QI[slot, x] = q[x] + IW[r, x]

        def relay_fields(r):
            relay(*conduct_args(r))
            relay(*inflow_args(r))

        relay(*pressure_args())
        relay(*storage_args())
        ids_handed().start()
        relay_fields(0)
        distribute(1)
        if R > 2:
            distribute(2)
        spread_here(*pressure_args())
        spread_here(*storage_args())
        for x in range(X):
            CW[H + (1 - h) * X + x] = looked_up(IR[H + (1 - h) * X + x], 0)
        for side in (0, 1):
            @pl.when(side_here[side])
            def _():
                first = H + XU if side else 1
                for x in range(first, first + H - 1):
                    CW[x] = looked_up(IR[x], 0)
        coefficients(0)
        relay_fields(1)

        def step(r, carry):
            slot = lax.rem(r, 2)

            def first(layers):
                for x in layers:
                    WW[0, x] = SA[r, x] * PB[r, x]

            def sweep_one(layers):
                for x in layers:
                    b = CW[x] * PB[r, x] + QI[slot, x]
                    d = SS[slot, x] * b
                    BB[x] = b
                    DD[x] = d
                    WW[1, x] = d + EE[slot, x] * neighbours(lambda y: WW[0, y], x)

            first(range(H, H + XU))
            sweep_one(range(H + 1, H + XU - 1))

            @pl.when(r > 0)
            def _():
                for side in (0, 1):
                    @pl.when(side_here[side])
                    def _():
                        part = PB.at[r, pl.ds(H + XU if side else 0, H)]
                        rdma(part, part, sP.at[r, side], rP.at[r, side], (t, pair)).wait_recv()

            first(range(0, H))
            sweep_one(range(1, H + 1))
            first(range(H + XU, WL))
            sweep_one(range(H + XU - 1, WL - 1))
            for j in range(1, ITERS - 1):
                for x in range(j + 1, WL - j - 1):
                    WW[j + 1, x] = DD[x] + EE[slot, x] * neighbours(lambda y: WW[j, y], x)

            def last(x):
                return RC[slot, x] * (
                    BB[x] + SA[r, x] * neighbours(lambda y: WW[ITERS - 1, y], x)
                )

            def send(side):
                @pl.when(jnp.logical_and(r < R - 1, side_here[side]))
                def _():
                    round_of(r + 1, side).start()

            for x in range(H, H + X):
                PB[r + 1, x] = last(x)
            send(0)
            for x in range(H + X, H + XU):
                PB[r + 1, x] = last(x)
            send(1)
            handed(r)[1].start()
            for half in (0, 1):
                put_out(r, half, PB.at[r + 1, pl.ds(H + half * X, X)], 0)
            PX[r, 0] = last(H - 1)
            PX[r, 1] = last(H + XU)
            handed(r)[2].start()
            seen = jnp.dot(pick_rows, PB[r + 1, H:H + XU].reshape(XU * Z, Y), precision=EXACT)
            predicted = jnp.sum(seen * pick_cols, axis=1, keepdims=True)
            lines = lax.broadcasted_iota(jnp.int32, SM.shape[1:], 0)
            seen_row = jnp.sum(jnp.where(lines == 1 + member, SM[r], 0.0), axis=0, keepdims=True)
            gap = predicted - upright(seen_row[:, :W])
            ES[...] = ES[...] + owned * gap * gap

            @pl.when(r == R - 1)
            def _():
                E0[...] = jnp.broadcast_to(jnp.sum(ES[...], axis=0, keepdims=True), E0.shape)
                for d in range(1, U):
                    peer = lax.rem(u + d, U)
                    rdma(E0, E1.at[u], s1.at[d], r1.at[u], (t, 2 * peer + h)).start()

            @pl.when(r < R - 1)
            def _():
                coefficients(r + 1)

            @pl.when(r < R - 2)
            def _():
                relay_fields(r + 2)

            @pl.when(r < R - 3)
            def _():
                distribute(r + 3)
            return carry

        lax.fori_loop(0, R, step, 0)
        E1[u] = E0[...]
        for d in range(1, U):
            peer = lax.rem(u + d, U)
            rdma(E1.at[peer], E1.at[peer], s1.at[d], r1.at[peer], (t, pair)).wait_recv()
        whole = E1[0]
        for n in range(1, U):
            whole = whole + E1[n]
        E2[member] = whole

        def plane(act):
            n = 0
            for d in range(T):
                for half in (0, 1):
                    if d == 0 and half == 0:
                        continue
                    dev = (lax.rem(t + d, T), i if half == 0 else pair)
                    act(rdma(E2.at[member], E2.at[member], s2.at[n], r2.at[member], dev))
                    n += 1

        plane(lambda copy: copy.start())
        misfit_here(True)
        outs_here()
        outs_sent(PB.at[0, pl.ds(0, X)], 0)
        plane(lambda copy: copy.wait_send())
        for d in range(1, U):
            peer = lax.rem(u + d, U)
            rdma(E0, E1.at[u], s1.at[d], r1.at[u], (t, 2 * peer + h)).wait_send()

        def done(r, c):
            spread_sent(*conduct_args(r))
            spread_sent(*inflow_args(r))
            for copy in handed(r):
                copy.wait_send()

            @pl.when(r > 0)
            def _():
                for side in (0, 1):
                    @pl.when(side_here[side])
                    def _():
                        round_of(r, side).wait_send()
            return c

        lax.fori_loop(0, R, done, 0)
        spread_sent(*pressure_args())
        spread_sent(*storage_args())
        ids_handed().wait_send()

    @pl.when(core == 0)
    def _():
        def fraction(s, v):
            sq = s * s
            rest = (1.0 - s) * (1.0 - s)
            return sq / (sq + v * rest)

        def edge_flow(r, side):
            src = FE.at[r, XU - 1 if side else 0]
            return rdma(
                src, HF.at[r, 1 - side], sHF.at[r, side], rHF.at[r, 1 - side], (t, i + 4 * side - 2)
            )

        def first_flow(act):
            for side in (0, 1):
                @pl.when(jnp.logical_and(side_here[side], h == side))
                def _():
                    src = FE.at[0, XU - 1 if side else 0]
                    for n, hop in ((0, 2), (1, 1)):
                        act(rdma(
                            src, HF.at[0, 1 - side], sHF.at[0, n], rHF.at[0, 1 - side],
                            (t, i + hop * (2 * side - 1)),
                        ))

        def prepare(start):
            for x in range(X):
                rock = IDW[start + x]
                v = looked_up(rock, 1)
                V[start + x] = v
                G[start + x] = 0.1 * looked_up(rock, 2)
                FE[0, start + x] = fraction(SB[0, start + x], v)

        def pair_copies():
            part = pl.ds(h * X, X)
            return (rdma(SB.at[0, part], SB.at[0, part], sA.at[0], rA.at[0], (t, pair)),)

        for side in (0, 1):
            @pl.when(jnp.logical_not(side_here[side]))
            def _():
                def clear(r, c):
                    HF[r, side] = zero
                    return c

                lax.fori_loop(0, R, clear, 0)

        s0_in.wait()
        ids_win.wait()
        prepare(h * X)
        mult_in.wait()
        infl_in.wait()
        meet()
        send_fields()
        first_flow(lambda copy: copy.start())
        for d, peer in others_t:
            small_to(d, peer).start()
        rows = put_rows(u * XU, XU)
        pl.semaphore_wait(go, 1)
        for copy in pair_copies():
            copy.start()
        def sources(r):
            small_here(r)
            q_all = source(r, rows, XU)
            for x in range(XU):
                Q[x] = q_all[x]

        sources(0)
        there = pl.ds((1 - h) * X, X)
        rdma(SB.at[0, there], SB.at[0, there], sA.at[0], rA.at[0], (t, pair)).wait_recv()
        rdma(IDW.at[there], IDW.at[there], sA.at[1], rA.at[1], (t, pair)).wait_recv()
        prepare((1 - h) * X)

        def step(r, carry):
            for copy in handed(r):
                copy.wait_recv()
            for side in (0, 1):
                @pl.when(side_here[side])
                def _():
                    part = HF.at[r, side]
                    rdma(part, part, sHF.at[r, side], rHF.at[r, side], (t, pair)).wait_recv()

            def p_of(x):
                return PX[r, 0] if x < 0 else (PX[r, 1] if x >= XU else PB[r + 1, H + x])

            def f_of(x):
                return HF[r, 0] if x < 0 else (HF[r, 1] if x >= XU else FE[r, x])

            def face(ai, aj, pi, pj, fi, fj):
                fall = pi - pj
                return ai * aj * fall * jnp.where(fall > 0, fi, fj)

            def across(x):
                return face(SA[r, H + x - 1], SA[r, H + x], p_of(x - 1), p_of(x), f_of(x - 1), f_of(x))

            def transport(x, low, high):
                a = SA[r, H + x]
                p = p_of(x)
                f = f_of(x)
                s = SB[r, x]
                q = Q[x]
                cz = jnp.where(zi < Z - 1, face(a, after(a, 0), p, after(p, 0), f, after(f, 0)), 0.0)
                cy = jnp.where(yi < Y - 1, face(a, after(a, 1), p, after(p, 1), f, after(f, 1)), 0.0)
                out = (high - low) + (cz - before(cz, 0)) + (cy - before(cy, 1))
                gained = jnp.maximum(q, 0.0) * (1.0 - s) - jnp.maximum(-q, 0.0) * f - out
                s = s + G[x] * gained
                SB[r + 1, x] = s
                FE[r + 1, x] = fraction(s, V[x])

            for side in (0, 1):
                x = XU - 1 if side else 0
                transport(x, across(x), across(x + 1))

                @pl.when(jnp.logical_and(r < R - 1, side_here[side]))
                def _():
                    edge_flow(r + 1, side).start()

            low = across(1)
            for x in range(1, XU - 1):
                high = across(x + 1)
                transport(x, low, high)
                low = high
                if x == X - 1:
                    put_out(r, 0, SB.at[r + 1, pl.ds(0, X)], 1)
            put_out(r, 1, SB.at[r + 1, pl.ds(X, X)], 1)

            @pl.when(r < R - 1)
            def _():
                sources(r + 1)
            return carry

        lax.fori_loop(0, R, step, 0)
        misfit_here(False)
        outs_here()
        outs_sent(SB.at[0, pl.ds(0, X)], 1)
        for copy in pair_copies():
            copy.wait_send()

        first_flow(lambda copy: copy.wait_send())

        def done(r, c):
            for side in (0, 1):
                @pl.when(side_here[side])
                def _():
                    edge_flow(r, side).wait_send()
            return c

        lax.fori_loop(1, R, done, 0)

    each_field(lambda copy: copy.wait_send())
    for d, peer in others_t:
        small_to(d, peer).wait_send()


def deliver(mis_in, p_in, s_in, mis_out, p_out, s_out, row, done):
    members = p_in.shape[1]
    copies = []
    for n, (src, dst) in enumerate(((p_in, p_out), (s_in, s_out))):
        for m in range(members):
            copies.append(pltpu.make_async_copy(src.at[0, m], dst.at[0, m], done.at[n * members + m]))
    for copy in copies:
        copy.start()
    row[...] = mis_in[0, :members]
    last = pltpu.make_async_copy(row, mis_out, done.at[2 * members])
    last.start()
    for copy in copies + [last]:
        copy.wait()


def body(
    perm_field, step_multiplier, inflow, start_pressure, start_saturation,
    region_ids, region_table, well_cells, well_rates, observed,
):
    T = lax.axis_size("tm")
    N = lax.axis_size("space")
    X, Z, Y = start_pressure.shape
    W = well_cells.shape[0]
    members = perm_field.shape[0]
    assert members == T and T % 2 == 0 and N % 2 == 0 and X >= H and step_multiplier.shape[0] == 1
    assert Y & (Y - 1) == 0
    R = T
    U = N // 2
    XU = 2 * X
    WL = XU + 2 * H
    f32 = jnp.float32
    cell = (Z, Y)
    block = (X, Z, Y)
    window = (WL, Z, Y)
    unit = (XU, Z, Y)

    def buf(*shape):
        return pltpu.VMEM(shape, f32)

    dma = pltpu.SemaphoreType.DMA
    vmem = pl.BlockSpec(memory_space=pltpu.VMEM)
    anyspace = pl.BlockSpec(memory_space=pl.ANY)
    out_shape = jax.ShapeDtypeStruct((1, members) + block, f32)
    mis, outp, outs = pl.pallas_call(
        functools.partial(kernel, T, N),
        out_shape=(pltpu.VMEM((8, 128), f32), pltpu.VMEM(out_shape.shape, f32), pltpu.VMEM(out_shape.shape, f32)),
        in_specs=[pl.BlockSpec(memory_space=pltpu.HBM)] * 6 + [pl.BlockSpec(memory_space=pltpu.SMEM)] + [vmem] * 3,
        out_specs=(vmem, vmem, vmem),
        scratch_shapes=[
            buf(2, *block), pltpu.VMEM(window, jnp.int32), buf(R, *block), buf(R, *window), buf(*window),
            buf(R, *window), buf(R, *block), buf(R + 1, *window), buf(R, 2, *cell), buf(T, 8 * (T // 8 + 1), 128),
            buf(2, *window), buf(2, *window), buf(2, *window), buf(2, *window), buf(*window),
            buf(*window), buf(ITERS, *window),
            pltpu.VMEM(unit, jnp.int32), buf(R + 1, *unit), buf(R + 1, *unit), buf(R, 2, *cell),
            buf(*unit), buf(*unit), buf(*unit), buf(W, 1), buf(8, 128), buf(U, 8, 128), buf(T, 8, 128),
            dma((5,)), dma((2, T // 2)), dma((2, T)), dma((2 * R + 2, 3)), dma((2 * R + 2, 3)),
            dma((R, 3)), dma((R, 3)), dma((R + 1, 2)), dma((R + 1, 2)), dma((T,)), dma((T,)),
            dma((2,)), dma((2,)), dma((R, 2)), dma((R, 2)),
            dma((R, 2)), dma((2, T)), dma(()), dma((max(U, 2),)), dma((U,)), dma((2 * T - 1,)), dma((T,)),
            pltpu.SemaphoreType.REGULAR,
        ],
        compiler_params=pltpu.CompilerParams(
            has_side_effects=True, collective_id=0, vmem_limit_bytes=56 * 1024 * 1024
        ),
    )(
        perm_field, step_multiplier, inflow, start_pressure, start_saturation, region_ids,
        region_table, well_cells[None], well_rates, observed[:, 0, :],
    )
    return pl.pallas_call(
        deliver,
        out_shape=(jax.ShapeDtypeStruct((members,), f32), out_shape, out_shape),
        in_specs=[vmem, vmem, vmem],
        out_specs=(anyspace, anyspace, anyspace),
        scratch_shapes=[buf(members), dma((2 * members + 1,))],
    )(
        pltpu.with_memory_space_constraint(mis, pltpu.VMEM),
        pltpu.with_memory_space_constraint(outp, pltpu.VMEM),
        pltpu.with_memory_space_constraint(outs, pltpu.VMEM),
    )


def solution(mesh):
    return jax.shard_map(
        body,
        mesh=mesh,
        in_specs=(
            P(None, "space", None, None),
            P("tm", "space", None, None),
            P("tm", "space", None, None),
            P("space", None, None),
            P("space", None, None),
            P("space", None, None),
            P(),
            P(),
            P("tm", None),
            P(None, "tm", None),
        ),
        out_specs=(P(), P("tm", None, "space", None, None), P("tm", None, "space", None, None)),
        check_vma=False,
    )
```

```python
import functools

import jax
import jax.numpy as jnp
from jax import lax
from jax.experimental import pallas as pl
from jax.experimental.pallas import tpu as pltpu
from jax.sharding import PartitionSpec as P

ITERS = 3
H = ITERS + 1
MESH = pl.DeviceIdType.MESH
EXACT = lax.Precision.HIGHEST


def before(v, axis):
    return pltpu.roll(v, 1, axis)


def after(v, axis):
    return pltpu.roll(v, v.shape[axis] - 1, axis)


def kernel(
    T, N,
    perm, mult, infl, p0, s0, ids, table, cells, rates, seen_in,
    mis, outp, outs,
    PM, IR, MS, IW, CW, SA, SO, PB, PX, SM, RC, SS, EE, QI, BB, DD, WW,
    IDW, SB, FE, HF, V, G, Q, ES, E0, E1, E2,
    lIN, sF, rF, sS, rS, sX, rX, sP, rP, sM, rM, sA, rA, sHF, rHF, sO, rO, lO, s1, r1, s2, r2,
):
    t = lax.axis_index("tm")
    i = lax.axis_index("space")
    X, Z, Y = p0.shape
    R = T
    W = cells.shape[1]
    U = N // 2
    XU = 2 * X
    WL = XU + 2 * H
    row = t // 2
    core = lax.rem(t, 2)
    u = i // 2
    h = lax.rem(i, 2)
    mate = t + 1 - 2 * core
    pair = i + 1 - 2 * h
    member = 2 * row + h
    own = H + h * X
    side_here = (u > 0, u < U - 1)

    def load(n, src, dst):
        return pltpu.make_async_copy(src, dst, lIN.at[n])

    def rdma(src, dst, ss, rs, dev):
        return pltpu.make_async_remote_copy(
            src_ref=src, dst_ref=dst, send_sem=ss, recv_sem=rs, device_id=dev, device_id_type=MESH
        )

    mult_in = load(0, mult.at[0], MS.at[t])
    infl_in = load(1, infl.at[0], IW.at[t, pl.ds(own, X)])
    ids_in = load(2, ids, IR.at[pl.ds(own, X)])
    perm_in = load(3, perm.at[pl.ds(2 * row, 2)], PM)
    p0_in = load(4, p0, PB.at[0, pl.ds(own, X)])
    s0_in = load(3, s0, SB.at[0, pl.ds(h * X, X)])
    ids_win = load(4, ids, IDW.at[pl.ds(h * X, X)])
    mult_in.start()
    infl_in.start()

    @pl.when(core == 1)
    def _():
        perm_in.start()
        p0_in.start()
        ids_in.start()

    @pl.when(core == 0)
    def _():
        s0_in.start()
        ids_win.start()

    barrier = pltpu.get_barrier_semaphore()

    def greet(device):
        pl.semaphore_signal(barrier, inc=1, device_id=device, device_id_type=MESH)

    for d in range(1, T):
        peer = lax.rem(t + d, T)
        greet((peer, i))
        greet((peer, pair))
    for d in range(1, N):
        greet((t, lax.rem(i + d, N)))

    zi = lax.broadcasted_iota(jnp.int32, (Z, Y), 0)
    yi = lax.broadcasted_iota(jnp.int32, (Z, Y), 1)
    zero = jnp.zeros((Z, Y), jnp.float32)

    def neighbours(at, x):
        w = at(x)
        total = at(x - 1) + at(x + 1)
        total = total + (
            jnp.where(zi < Z - 1, after(w, 0), 0.0) + jnp.where(zi > 0, before(w, 0), 0.0)
        )
        return total + (
            jnp.where(yi < Y - 1, after(w, 1), 0.0) + jnp.where(yi > 0, before(w, 1), 0.0)
        )

    def looked_up(rock, which):
        v = zero
        for k in range(table.shape[1]):
            v = jnp.where(rock == k, table[which, k], v)
        return v

    def upright(line):
        eye = lax.broadcasted_iota(jnp.int32, (W, W), 0) == lax.broadcasted_iota(jnp.int32, (W, W), 1)
        return jnp.sum(jnp.where(eye, line, 0.0), axis=1, keepdims=True)

    bits = Y.bit_length() - 1
    rows_row = jnp.right_shift(cells[...], bits).astype(jnp.float32)
    cols_row = jnp.bitwise_and(cells[...], Y - 1).astype(jnp.float32)
    pick_cols = jnp.where(
        lax.broadcasted_iota(jnp.int32, (W, Y), 1).astype(jnp.float32) == upright(cols_row), 1.0, 0.0
    )
    SM[t] = jnp.zeros(SM.shape[1:], jnp.float32)
    SM[t, 0:1, 0:W] = rates[...]
    SM[t, 1:1 + T, 0:W] = seen_in[...]

    def put_rows(first, count):
        base = (first * Z).astype(jnp.float32)
        return jnp.where(
            lax.broadcasted_iota(jnp.int32, (count * Z, W), 0).astype(jnp.float32) == rows_row - base,
            1.0, 0.0,
        )

    others_t = [(d, lax.rem(t + d, T)) for d in range(1, T)]

    def small_to(d, peer):
        return rdma(SM.at[t], SM.at[t], sM.at[d], rM.at[t], (peer, i))

    def small_here(r):
        @pl.when(r != t)
        def _():
            rdma(SM.at[r], SM.at[r], sM.at[1], rM.at[r], (r, i)).wait_recv()

    def source(r, rows, count):
        rate = upright(SM[r, 0:1, 0:W])
        return jnp.dot(rows, pick_cols * rate, precision=EXACT).reshape(count, Z, Y)

    def field_to(rr):
        dev = (2 * rr + 1, i)
        return (
            rdma(MS.at[t], MS.at[t], sF.at[0, rr], rF.at[0, t], dev),
            rdma(
                IW.at[t, pl.ds(own, X)], IW.at[t, pl.ds(own, X)], sF.at[1, rr], rF.at[1, t], dev
            ),
        )

    def each_field(act):
        for rr in range(T // 2):
            @pl.when(t != 2 * rr + 1)
            def _():
                for copy in field_to(rr):
                    act(copy)

    def send_fields():
        each_field(lambda copy: copy.start())

    def put_out(r, half, src, which):
        dst = (outp, outs)[which].at[0, member]
        here = jnp.logical_and(r == t, half == h)

        @pl.when(jnp.logical_not(here))
        def _():
            rdma(src, dst, sO.at[r, half], rO.at[which, member], (r, 2 * u + half)).start()

        @pl.when(here)
        def _():
            pltpu.make_async_copy(src, dst, lO).start()

    def outs_sent(src, which):
        def sent(r, c):
            for half in (0, 1):
                dst = (outp, outs)[which].at[0, member]
                here = jnp.logical_and(r == t, half == h)

                @pl.when(jnp.logical_not(here))
                def _():
                    rdma(src, dst, sO.at[r, half], rO.at[which, member], (r, 2 * u + half)).wait_send()
            return c

        lax.fori_loop(0, R, sent, 0)
        pltpu.make_async_copy(src, (outp, outs)[which].at[0, member], lO).wait()

    def outs_here():
        for which in (0, 1):
            for m in range(T):
                mine = jnp.logical_and(core == 1 - which, m == member)

                @pl.when(jnp.logical_not(mine))
                def _():
                    dst = (outp, outs)[which].at[0, m]
                    rdma(dst, dst, sO.at[0, 0], rO.at[which, m], (t, pair)).wait_recv()

    def misfit_here(skip):
        for m in range(T):
            wait = rdma(E2.at[m], E2.at[m], s2.at[0], r2.at[m], (t, pair))
            if skip:
                @pl.when(m != member)
                def _():
                    wait.wait_recv()
            else:
                wait.wait_recv()
        lanes = lax.broadcasted_iota(jnp.int32, (8, 128), 1)
        result = jnp.zeros((8, 128), jnp.float32)
        for m in range(T):
            result = result + jnp.where(lanes == m, E2[m], 0.0)
        mis[...] = result * (1.0 / (R * W))

    def edge_of(side, depth):
        src = pl.ds(H + XU - depth if side else H, depth)
        dst = pl.ds(H - depth if side else H + XU, depth)
        return src, dst

    def pooled(n, window, other):
        return rdma(
            other.at[pl.ds(0, X)], window.at[pl.ds(own, X)], sS.at[n, 0], rS.at[n, 0], (t, pair)
        )

    def halo(n, window, depth, side, relayed):
        src, dst = edge_of(side, depth)
        return rdma(
            window.at[src], window.at[dst], sS.at[n, 1 + relayed], rS.at[n, 2 - side],
            (t, i + 4 * side - 2),
        )

    def halos(n, window, depth, relayed, act):
        for side in (0, 1):
            @pl.when(jnp.logical_and(side_here[side], h == (1 - side if relayed else side)))
            def _():
                act(halo(n, window, depth, side, relayed))

    def pool(n, window, depth, other):
        pooled(n, window, other).start()
        halos(n, window, depth, 0, lambda copy: copy.start())

    def relay(n, window, depth, other):
        part = window.at[pl.ds(H + (1 - h) * X, X)]
        rdma(part, part, sS.at[n, 0], rS.at[n, 0], (t, pair)).wait_recv()
        halos(n, window, depth, 1, lambda copy: copy.start())

    def spread_here(n, window, depth, other):
        for side in (0, 1):
            @pl.when(side_here[side])
            def _():
                part = window.at[pl.ds(H + XU if side else H - depth, depth)]
                rdma(part, part, sS.at[n, 1], rS.at[n, 1 + side], (t, pair)).wait_recv()

    def spread_sent(n, window, depth, other):
        pooled(n, window, other).wait_send()
        for relayed in (0, 1):
            halos(n, window, depth, relayed, lambda copy: copy.wait_send())

    def own_of(window):
        return window.at[pl.ds(own, X)]

    def conduct_args(r):
        return r, SA.at[r], H, SO.at[r]

    def inflow_args(r):
        return R + r, IW.at[r], H - 1, own_of(IW.at[r])

    def pressure_args():
        return 2 * R, PB.at[0], H, own_of(PB.at[0])

    def storage_args():
        return 2 * R + 1, IR, H - 1, own_of(IR)

    def distribute(r):
        @pl.when(r != t)
        def _():
            rdma(MS.at[r], MS.at[r], sF.at[0, 0], rF.at[0, r], (r, i)).wait_recv()

        for x in range(X):
            SO[r, x] = jnp.sqrt(PM[1 - h, x] * MS[r, x])
            SA[r, own + x] = jnp.sqrt(PM[h, x] * MS[r, x])
        pool(*conduct_args(r))

        @pl.when(r != t)
        def _():
            mine = own_of(IW.at[r])
            rdma(mine, mine, sF.at[1, 0], rF.at[1, r], (r, i)).wait_recv()
        pool(*inflow_args(r))

    def round_of(k, side):
        if side == 0:
            src, dst, dev = pl.ds(H, H), pl.ds(H + XU, H), (t, i - 2)
        else:
            src, dst, dev = pl.ds(XU, H), pl.ds(0, H), (t, i + 2)
        return rdma(PB.at[k, src], PB.at[k, dst], sP.at[k, side], rP.at[k, 1 - side], dev)

    def handed(r):
        mid = pl.ds(H, XU)
        wide = pl.ds(H - 1, XU + 2)
        dev = (mate, i)
        return (
            rdma(SA.at[r, wide], SA.at[r, wide], sX.at[r, 0], rX.at[r, 0], dev),
            rdma(PB.at[r + 1, mid], PB.at[r + 1, mid], sX.at[r, 1], rX.at[r, 1], dev),
            rdma(PX.at[r], PX.at[r], sX.at[r, 2], rX.at[r, 2], dev),
        )

    def ids_handed():
        return rdma(
            IR.at[pl.ds(H + (1 - h) * X, X)], IDW.at[pl.ds((1 - h) * X, X)], sA.at[1], rA.at[1], (mate, i)
        )

    def meet():
        pl.semaphore_wait(barrier, (N - 1) + 2 * (T - 1))

    @pl.when(core == 1)
    def _():
        ids_in.wait()
        for x in range(X):
            CW[own + x] = looked_up(IR[own + x], 0)
        for side in (0, 1):
            @pl.when(jnp.logical_not(side_here[side]))
            def _():
                first = H + XU if side else 0
                for x in range(first, first + H):
                    CW[x] = zero + 1.0

                def clear(r, c):
                    for x in range(first, first + H):
                        SA[r, x] = zero
                        IW[r, x] = zero
                        PB[r, x] = zero
                    return c

                lax.fori_loop(0, R, clear, 0)
        p0_in.wait()
        mult_in.wait()
        infl_in.wait()
        perm_in.wait()
        meet()
        pool(*pressure_args())
        pool(*storage_args())
        for d, peer in others_t:
            small_to(d, peer).start()
        distribute(0)
        send_fields()
        rows = put_rows(u * XU - H, WL)
        local = upright(rows_row) - (u * (XU * Z)).astype(jnp.float32)
        pick_rows = jnp.where(
            lax.broadcasted_iota(jnp.int32, (W, XU * Z), 1).astype(jnp.float32) == local, 1.0, 0.0
        )
        owned = jnp.sum(pick_rows, axis=1, keepdims=True)
        ES[...] = jnp.zeros(ES.shape, jnp.float32)

        def coefficients(r):
            slot = lax.rem(r, 2)
            spread_here(*conduct_args(r))
            handed(r)[0].start()
            for x in range(1, WL - 1):
                a = SA[r, x]
                rc = 1.0 / (CW[x] + a * neighbours(lambda y: SA[r, y], x))
                RC[slot, x] = rc
                ss = a * rc
                SS[slot, x] = ss
                EE[slot, x] = a * ss
            small_here(r)
            q = source(r, rows, WL)
            spread_here(*inflow_args(r))
            for x in range(1, WL - 1):
                QI[slot, x] = q[x] + IW[r, x]

        def relay_fields(r):
            relay(*conduct_args(r))
            relay(*inflow_args(r))

        relay(*pressure_args())
        relay(*storage_args())
        ids_handed().start()
        relay_fields(0)
        distribute(1)
        if R > 2:
            distribute(2)
        spread_here(*pressure_args())
        spread_here(*storage_args())
        for x in range(X):
            CW[H + (1 - h) * X + x] = looked_up(IR[H + (1 - h) * X + x], 0)
        for side in (0, 1):
            @pl.when(side_here[side])
            def _():
                first = H + XU if side else 1
                for x in range(first, first + H - 1):
                    CW[x] = looked_up(IR[x], 0)
        coefficients(0)
        relay_fields(1)

        def step(r, carry):
            slot = lax.rem(r, 2)

            def first(layers):
                for x in layers:
                    WW[0, x] = SA[r, x] * PB[r, x]

            def sweep_one(layers):
                for x in layers:
                    b = CW[x] * PB[r, x] + QI[slot, x]
                    d = SS[slot, x] * b
                    BB[x] = b
                    DD[x] = d
                    WW[1, x] = d + EE[slot, x] * neighbours(lambda y: WW[0, y], x)

            first(range(H, H + XU))
            sweep_one(range(H + 1, H + XU - 1))

            @pl.when(r > 0)
            def _():
                for side in (0, 1):
                    @pl.when(side_here[side])
                    def _():
                        part = PB.at[r, pl.ds(H + XU if side else 0, H)]
                        rdma(part, part, sP.at[r, side], rP.at[r, side], (t, pair)).wait_recv()

            first(range(0, H))
            sweep_one(range(1, H + 1))
            first(range(H + XU, WL))
            sweep_one(range(H + XU - 1, WL - 1))
            for j in range(1, ITERS - 1):
                for x in range(j + 1, WL - j - 1):
                    WW[j + 1, x] = DD[x] + EE[slot, x] * neighbours(lambda y: WW[j, y], x)

            def last(x):
                return RC[slot, x] * (
                    BB[x] + SA[r, x] * neighbours(lambda y: WW[ITERS - 1, y], x)
                )

            def send(side):
                @pl.when(jnp.logical_and(r < R - 1, side_here[side]))
                def _():
                    round_of(r + 1, side).start()

            for x in range(H, H + X):
                PB[r + 1, x] = last(x)
            send(0)
            for x in range(H + X, H + XU):
                PB[r + 1, x] = last(x)
            send(1)
            handed(r)[1].start()
            for half in (0, 1):
                put_out(r, half, PB.at[r + 1, pl.ds(H + half * X, X)], 0)
            PX[r, 0] = last(H - 1)
            PX[r, 1] = last(H + XU)
            handed(r)[2].start()
            seen = jnp.dot(pick_rows, PB[r + 1, H:H + XU].reshape(XU * Z, Y), precision=EXACT)
            predicted = jnp.sum(seen * pick_cols, axis=1, keepdims=True)
            lines = lax.broadcasted_iota(jnp.int32, SM.shape[1:], 0)
            seen_row = jnp.sum(jnp.where(lines == 1 + member, SM[r], 0.0), axis=0, keepdims=True)
            gap = predicted - upright(seen_row[:, :W])
            ES[...] = ES[...] + owned * gap * gap

            @pl.when(r == R - 1)
            def _():
                E0[...] = jnp.broadcast_to(jnp.sum(ES[...], axis=0, keepdims=True), E0.shape)
                for d in range(1, U):
                    peer = lax.rem(u + d, U)
                    rdma(E0, E1.at[u], s1.at[d], r1.at[u], (t, 2 * peer + h)).start()

            @pl.when(r < R - 1)
            def _():
                coefficients(r + 1)

            @pl.when(r < R - 2)
            def _():
                relay_fields(r + 2)

            @pl.when(r < R - 3)
            def _():
                distribute(r + 3)
            return carry

        lax.fori_loop(0, R, step, 0)
        E1[u] = E0[...]
        for d in range(1, U):
            peer = lax.rem(u + d, U)
            rdma(E1.at[peer], E1.at[peer], s1.at[d], r1.at[peer], (t, pair)).wait_recv()
        whole = E1[0]
        for n in range(1, U):
            whole = whole + E1[n]
        E2[member] = whole

        def plane(act):
            n = 0
            for d in range(T):
                for half in (0, 1):
                    if d == 0 and half == 0:
                        continue
                    dev = (lax.rem(t + d, T), i if half == 0 else pair)
                    act(rdma(E2.at[member], E2.at[member], s2.at[n], r2.at[member], dev))
                    n += 1

        plane(lambda copy: copy.start())
        misfit_here(True)
        outs_here()
        outs_sent(PB.at[0, pl.ds(0, X)], 0)
        plane(lambda copy: copy.wait_send())
        for d in range(1, U):
            peer = lax.rem(u + d, U)
            rdma(E0, E1.at[u], s1.at[d], r1.at[u], (t, 2 * peer + h)).wait_send()

        def done(r, c):
            spread_sent(*conduct_args(r))
            spread_sent(*inflow_args(r))
            for copy in handed(r):
                copy.wait_send()

            @pl.when(r > 0)
            def _():
                for side in (0, 1):
                    @pl.when(side_here[side])
                    def _():
                        round_of(r, side).wait_send()
            return c

        lax.fori_loop(0, R, done, 0)
        spread_sent(*pressure_args())
        spread_sent(*storage_args())
        ids_handed().wait_send()

    @pl.when(core == 0)
    def _():
        def fraction(s, v):
            sq = s * s
            rest = (1.0 - s) * (1.0 - s)
            return sq / (sq + v * rest)

        def edge_flow(r, side):
            src = FE.at[r, XU - 1 if side else 0]
            return rdma(
                src, HF.at[r, 1 - side], sHF.at[r, side], rHF.at[r, 1 - side], (t, i + 4 * side - 2)
            )

        def first_flow(act):
            for side in (0, 1):
                @pl.when(jnp.logical_and(side_here[side], h == side))
                def _():
                    src = FE.at[0, XU - 1 if side else 0]
                    for n, hop in ((0, 2), (1, 1)):
                        act(rdma(
                            src, HF.at[0, 1 - side], sHF.at[0, n], rHF.at[0, 1 - side],
                            (t, i + hop * (2 * side - 1)),
                        ))

        def prepare(start):
            for x in range(X):
                rock = IDW[start + x]
                v = looked_up(rock, 1)
                V[start + x] = v
                G[start + x] = 0.1 * looked_up(rock, 2)
                FE[0, start + x] = fraction(SB[0, start + x], v)

        def pair_copies():
            part = pl.ds(h * X, X)
            return (rdma(SB.at[0, part], SB.at[0, part], sA.at[0], rA.at[0], (t, pair)),)

        for side in (0, 1):
            @pl.when(jnp.logical_not(side_here[side]))
            def _():
                def clear(r, c):
                    HF[r, side] = zero
                    return c

                lax.fori_loop(0, R, clear, 0)

        s0_in.wait()
        ids_win.wait()
        prepare(h * X)
        mult_in.wait()
        infl_in.wait()
        meet()
        send_fields()
        first_flow(lambda copy: copy.start())
        for d, peer in others_t:
            small_to(d, peer).start()
        rows = put_rows(u * XU, XU)
        for copy in pair_copies():
            copy.start()
        def sources(r):
            small_here(r)
            q_all = source(r, rows, XU)
            for x in range(XU):
                Q[x] = q_all[x]

        sources(0)
        there = pl.ds((1 - h) * X, X)
        rdma(SB.at[0, there], SB.at[0, there], sA.at[0], rA.at[0], (t, pair)).wait_recv()
        rdma(IDW.at[there], IDW.at[there], sA.at[1], rA.at[1], (t, pair)).wait_recv()
        prepare((1 - h) * X)

        def step(r, carry):
            for copy in handed(r):
                copy.wait_recv()
            for side in (0, 1):
                @pl.when(side_here[side])
                def _():
                    part = HF.at[r, side]
                    rdma(part, part, sHF.at[r, side], rHF.at[r, side], (t, pair)).wait_recv()

            def p_of(x):
                return PX[r, 0] if x < 0 else (PX[r, 1] if x >= XU else PB[r + 1, H + x])

            def f_of(x):
                return HF[r, 0] if x < 0 else (HF[r, 1] if x >= XU else FE[r, x])

            def face(ai, aj, pi, pj, fi, fj):
                fall = pi - pj
                return ai * aj * fall * jnp.where(fall > 0, fi, fj)

            def across(x):
                return face(SA[r, H + x - 1], SA[r, H + x], p_of(x - 1), p_of(x), f_of(x - 1), f_of(x))

            def transport(x, low, high):
                a = SA[r, H + x]
                p = p_of(x)
                f = f_of(x)
                s = SB[r, x]
                q = Q[x]
                cz = jnp.where(zi < Z - 1, face(a, after(a, 0), p, after(p, 0), f, after(f, 0)), 0.0)
                cy = jnp.where(yi < Y - 1, face(a, after(a, 1), p, after(p, 1), f, after(f, 1)), 0.0)
                out = (high - low) + (cz - before(cz, 0)) + (cy - before(cy, 1))
                gained = jnp.maximum(q, 0.0) * (1.0 - s) - jnp.maximum(-q, 0.0) * f - out
                s = s + G[x] * gained
                SB[r + 1, x] = s
                FE[r + 1, x] = fraction(s, V[x])

            for side in (0, 1):
                x = XU - 1 if side else 0
                transport(x, across(x), across(x + 1))

                @pl.when(jnp.logical_and(r < R - 1, side_here[side]))
                def _():
                    edge_flow(r + 1, side).start()

            low = across(1)
            for x in range(1, XU - 1):
                high = across(x + 1)
                transport(x, low, high)
                low = high
                if x == X - 1:
                    put_out(r, 0, SB.at[r + 1, pl.ds(0, X)], 1)
            put_out(r, 1, SB.at[r + 1, pl.ds(X, X)], 1)

            @pl.when(r < R - 1)
            def _():
                sources(r + 1)
            return carry

        lax.fori_loop(0, R, step, 0)
        misfit_here(False)
        outs_here()
        outs_sent(SB.at[0, pl.ds(0, X)], 1)
        for copy in pair_copies():
            copy.wait_send()

        first_flow(lambda copy: copy.wait_send())

        def done(r, c):
            for side in (0, 1):
                @pl.when(side_here[side])
                def _():
                    edge_flow(r, side).wait_send()
            return c

        lax.fori_loop(1, R, done, 0)

    each_field(lambda copy: copy.wait_send())
    for d, peer in others_t:
        small_to(d, peer).wait_send()


def deliver(mis_in, p_in, s_in, mis_out, p_out, s_out, row, done):
    members = p_in.shape[1]
    copies = []
    for n, (src, dst) in enumerate(((p_in, p_out), (s_in, s_out))):
        for m in range(members):
            copies.append(pltpu.make_async_copy(src.at[0, m], dst.at[0, m], done.at[n * members + m]))
    for copy in copies:
        copy.start()
    row[...] = mis_in[0, :members]
    last = pltpu.make_async_copy(row, mis_out, done.at[2 * members])
    last.start()
    for copy in copies + [last]:
        copy.wait()


def body(
    perm_field, step_multiplier, inflow, start_pressure, start_saturation,
    region_ids, region_table, well_cells, well_rates, observed,
):
    T = lax.axis_size("tm")
    N = lax.axis_size("space")
    X, Z, Y = start_pressure.shape
    W = well_cells.shape[0]
    members = perm_field.shape[0]
    assert members == T and T % 2 == 0 and N % 2 == 0 and X >= H and step_multiplier.shape[0] == 1
    assert Y & (Y - 1) == 0
    R = T
    U = N // 2
    XU = 2 * X
    WL = XU + 2 * H
    f32 = jnp.float32
    cell = (Z, Y)
    block = (X, Z, Y)
    window = (WL, Z, Y)
    unit = (XU, Z, Y)

    def buf(*shape):
        return pltpu.VMEM(shape, f32)

    dma = pltpu.SemaphoreType.DMA
    vmem = pl.BlockSpec(memory_space=pltpu.VMEM)
    anyspace = pl.BlockSpec(memory_space=pl.ANY)
    out_shape = jax.ShapeDtypeStruct((1, members) + block, f32)
    mis, outp, outs = pl.pallas_call(
        functools.partial(kernel, T, N),
        out_shape=(pltpu.VMEM((8, 128), f32), pltpu.VMEM(out_shape.shape, f32), pltpu.VMEM(out_shape.shape, f32)),
        in_specs=[pl.BlockSpec(memory_space=pltpu.HBM)] * 6 + [pl.BlockSpec(memory_space=pltpu.SMEM)] + [vmem] * 3,
        out_specs=(vmem, vmem, vmem),
        scratch_shapes=[
            buf(2, *block), pltpu.VMEM(window, jnp.int32), buf(R, *block), buf(R, *window), buf(*window),
            buf(R, *window), buf(R, *block), buf(R + 1, *window), buf(R, 2, *cell), buf(T, 8 * (T // 8 + 1), 128),
            buf(2, *window), buf(2, *window), buf(2, *window), buf(2, *window), buf(*window),
            buf(*window), buf(ITERS, *window),
            pltpu.VMEM(unit, jnp.int32), buf(R + 1, *unit), buf(R + 1, *unit), buf(R, 2, *cell),
            buf(*unit), buf(*unit), buf(*unit), buf(W, 1), buf(8, 128), buf(U, 8, 128), buf(T, 8, 128),
            dma((5,)), dma((2, T // 2)), dma((2, T)), dma((2 * R + 2, 3)), dma((2 * R + 2, 3)),
            dma((R, 3)), dma((R, 3)), dma((R + 1, 2)), dma((R + 1, 2)), dma((T,)), dma((T,)),
            dma((2,)), dma((2,)), dma((R, 2)), dma((R, 2)),
            dma((R, 2)), dma((2, T)), dma(()), dma((max(U, 2),)), dma((U,)), dma((2 * T - 1,)), dma((T,)),
        ],
        compiler_params=pltpu.CompilerParams(
            has_side_effects=True, collective_id=0, vmem_limit_bytes=56 * 1024 * 1024
        ),
    )(
        perm_field, step_multiplier, inflow, start_pressure, start_saturation, region_ids,
        region_table, well_cells[None], well_rates, observed[:, 0, :],
    )
    return pl.pallas_call(
        deliver,
        out_shape=(jax.ShapeDtypeStruct((members,), f32), out_shape, out_shape),
        in_specs=[vmem, vmem, vmem],
        out_specs=(anyspace, anyspace, anyspace),
        scratch_shapes=[buf(members), dma((2 * members + 1,))],
    )(
        pltpu.with_memory_space_constraint(mis, pltpu.VMEM),
        pltpu.with_memory_space_constraint(outp, pltpu.VMEM),
        pltpu.with_memory_space_constraint(outs, pltpu.VMEM),
    )


def solution(mesh):
    return jax.shard_map(
        body,
        mesh=mesh,
        in_specs=(
            P(None, "space", None, None),
            P("tm", "space", None, None),
            P("tm", "space", None, None),
            P("space", None, None),
            P("space", None, None),
            P("space", None, None),
            P(),
            P(),
            P("tm", None),
            P(None, "tm", None),
        ),
        out_specs=(P(), P("tm", None, "space", None, None), P("tm", None, "space", None, None)),
        check_vma=False,
    )
```
